8 devices in a mesh: dp: 1 (over z), ep: 8 (over y, x, core).
Axes of the slice: x: 2, y: 2, z: 1, core: 2. Of those that a mesh axis runs over, the one named last changes fastest.
Arguments:
- hidden: bfloat16 [768, 2048], P(('dp', 'ep'))
- norm_gain: bfloat16 [2048], replicated
- w_gate: bfloat16 [2048, 64], replicated
- w1_shared: bfloat16 [2048, 2816], replicated
- w3_shared: bfloat16 [2048, 2816], replicated
- w2_shared: bfloat16 [2816, 2048], replicated
- w1_experts: bfloat16 [64, 2048, 1408], P('ep')
- w3_experts: bfloat16 [64, 2048, 1408], P('ep')
- w2_experts: bfloat16 [64, 1408, 2048], P('ep')
- topk_ids: int32 [768, 6], P(('dp', 'ep'))
Outputs:
- output: bfloat16 [768, 2048], P(('dp', 'ep'))
All inputs are finite; a program needn't handle non-finite values.
Results may differ from the reference program's by a relative error of at most 0.00589404.
Values are sent between devices in bfloat16 or wider.
A program may use at most 1 GiB of HBM per device.

```python
import jax
import jax.numpy as jnp
from jax import lax

HIDDEN = 2048
EXPERTS = 64
EXPERT_FF = 1408
SHARED_FF = 2816
TOP_K = 6
TOKENS_DEV = 96
TOKENS = 768
GROUPS = 8
TOP_GROUPS = 3
ROUTE_SCALE = 16
NORM_EPS = 1e-6
GROUP_SIZE = EXPERTS // GROUPS


def draw_routing(route_key):
    blocks = TOKENS // TOKENS_DEV
    half_block = TOKENS_DEV // 2
    key_hot, key_cycle, key_perm, key_score, key_pick = jax.random.split(route_key, 5)
    hot_group = jax.random.randint(key_hot, (blocks, 1, 1), 0, GROUPS)
    cycle_off = jax.random.randint(key_cycle, (blocks, 1, 1), 0, GROUPS - 1)
    perm_keys = jax.random.split(key_perm, blocks)
    rank_in = jax.vmap(lambda sub_key: jax.random.permutation(sub_key, TOKENS_DEV))(perm_keys)[:, :, None]
    first_set = (rank_in * (TOP_GROUPS - 1) + jnp.arange(TOP_GROUPS - 1) + cycle_off) % (GROUPS - 1)
    first_groups = jnp.concatenate([jnp.broadcast_to(hot_group, (blocks, TOKENS_DEV, 1)), (hot_group + 1 + first_set) % GROUPS], axis=2)
    second_set = (rank_in * TOP_GROUPS + jnp.arange(TOP_GROUPS) + cycle_off) % (GROUPS - 1)
    second_groups = (hot_group + 1 + second_set) % GROUPS
    chosen = jnp.where(rank_in < half_block, first_groups, second_groups).reshape(TOKENS, TOP_GROUPS)
    scores = jax.random.randint(key_score, (TOKENS, TOP_GROUPS, GROUP_SIZE), 0, 2 ** 19) * 512
    scores = scores + jnp.arange(TOP_GROUPS * GROUP_SIZE).reshape(TOP_GROUPS, GROUP_SIZE)
    pick_idx = jax.random.randint(key_pick, (TOKENS, TOP_GROUPS, 1), 0, GROUP_SIZE)
    scores = scores + jnp.where(jnp.arange(GROUP_SIZE) == pick_idx, 2 ** 29, 0)
    cand_idx = lax.top_k(scores.reshape(TOKENS, TOP_GROUPS * GROUP_SIZE), TOP_K)[1]
    group_of = jnp.take_along_axis(chosen, cand_idx // GROUP_SIZE, axis=1)
    return (group_of * GROUP_SIZE + cand_idx % GROUP_SIZE).astype(jnp.int32)


def normal_bf16(sub_key, shape_in, scale_by):
    return (scale_by * jax.random.normal(sub_key, shape_in, jnp.float32)).astype(jnp.bfloat16)


def setup_inputs(seed: int = 0, part: int = 0) -> dict:
    part_key = jax.random.fold_in(jax.random.key(seed), part)
    weight_keys = jax.random.split(jax.random.key(seed + 1), 8)
    hidden = normal_bf16(jax.random.fold_in(part_key, 1), (TOKENS, HIDDEN), 0.5)
    norm_gain = (1.0 + 0.2 * jax.random.normal(weight_keys[0], (HIDDEN,), jnp.float32)).astype(jnp.bfloat16)
    w_gate = normal_bf16(weight_keys[1], (HIDDEN, EXPERTS), HIDDEN ** -0.5)
    w1_shared = normal_bf16(weight_keys[2], (HIDDEN, SHARED_FF), HIDDEN ** -0.5)
    w3_shared = normal_bf16(weight_keys[3], (HIDDEN, SHARED_FF), HIDDEN ** -0.5)
    w2_shared = normal_bf16(weight_keys[4], (SHARED_FF, HIDDEN), SHARED_FF ** -0.5)
    w1_experts = normal_bf16(weight_keys[5], (EXPERTS, HIDDEN, EXPERT_FF), HIDDEN ** -0.5)
    w3_experts = normal_bf16(weight_keys[6], (EXPERTS, HIDDEN, EXPERT_FF), HIDDEN ** -0.5)
    w2_experts = normal_bf16(weight_keys[7], (EXPERTS, EXPERT_FF, HIDDEN), EXPERT_FF ** -0.5)
    topk_ids = draw_routing(jax.random.fold_in(part_key, 2))
    return dict(hidden=hidden, norm_gain=norm_gain, w_gate=w_gate, w1_shared=w1_shared, w3_shared=w3_shared, w2_shared=w2_shared, w1_experts=w1_experts, w3_experts=w3_experts, w2_experts=w2_experts, topk_ids=topk_ids)


def rms_norm(hidden, norm_gain):
    rows_f = hidden.astype(jnp.float32)
    inv_rms = lax.rsqrt(jnp.mean(rows_f * rows_f, axis=-1, keepdims=True) + NORM_EPS)
    return (rows_f * inv_rms * norm_gain.astype(jnp.float32)).astype(jnp.bfloat16)


def swiglu(rows_in, w_up, w_lin, w_down):
    gate_act = jnp.dot(rows_in, w_up, preferred_element_type=jnp.float32)
    lin_act = jnp.dot(rows_in, w_lin, preferred_element_type=jnp.float32)
    inner_act = (jax.nn.silu(gate_act) * lin_act).astype(jnp.bfloat16)
    return jnp.dot(inner_act, w_down, preferred_element_type=jnp.float32).astype(jnp.bfloat16)


def reference(hidden, norm_gain, w_gate, w1_shared, w3_shared, w2_shared, w1_experts, w3_experts, w2_experts, topk_ids):
    normed = rms_norm(hidden, norm_gain)
    gate_probs = jax.nn.softmax(jnp.dot(normed, w_gate, preferred_element_type=jnp.float32), axis=-1)
    gate_wts = ROUTE_SCALE * jnp.take_along_axis(gate_probs, topk_ids, axis=1)
    shared_out = swiglu(normed, w1_shared, w3_shared, w2_shared)

    def expert_step(routed_acc, expert_in):
        w_up, w_lin, w_down, expert_id = expert_in
        column = jnp.sum(jnp.where(topk_ids == expert_id, gate_wts, 0.0), axis=1)
        expert_out = swiglu(normed, w_up, w_lin, w_down)
        return routed_acc + column[:, None] * expert_out.astype(jnp.float32), None

    routed = lax.scan(expert_step, jnp.zeros(hidden.shape, jnp.float32), (w1_experts, w3_experts, w2_experts, jnp.arange(EXPERTS)))[0]
    return (hidden.astype(jnp.float32) + shared_out.astype(jnp.float32) + routed).astype(jnp.bfloat16)
```

```python
import functools

import jax
import jax.numpy as jnp
from jax import lax
from jax.experimental import pallas as pl
from jax.experimental.pallas import tpu as pltpu
from jax.sharding import PartitionSpec as P

ROUTE_SCALE = 16
NORM_EPS = 1e-6
CAP = 128
CHUNK = 256
RING = 3
F32 = jnp.float32
BF16 = jnp.bfloat16


def dot_f32(lhs, rhs):
    return jnp.dot(lhs, rhs, preferred_element_type=F32)


def moe_kernel(base_ref, gain_ref, wgt_ref, idst_ref, y_hbm, w1s, w3s, w2s, w1e, w3e, w2e,
               out_ref, load_ref,
               y_ref, slots, ball, vall, vt_ref, rk_ref, tr_ref, q_all, xg_ref, act_ref, act_s,
               pbuf, dbuf, abuf, rbuf, sbuf,
               y_sem, wsem, ssem, rsem, ds_sem, dr_sem, as_sem, ar_sem, bs_sem, br_sem):
    rows = y_ref.shape[0]
    half = rows // 2
    experts, _, ff = w1e.shape
    chunks = w2e.shape[2] // CHUNK
    tokens = rows * 8
    me = lax.axis_index("ep")
    core = me % 2
    chip = me // 2
    xpos = chip % 2
    ypos = chip // 2
    partner = me + 1 - 2 * core
    xdev = me + 2 - 4 * xpos
    ydev = me + 4 - 8 * ypos
    xq = chip + 1 - 2 * xpos
    yq = chip + 2 - 4 * ypos
    dq = 3 - chip
    my_pos = core * 4 + chip
    x_pos = core * 4 + xq
    y_pos = core * 4 + yq
    d_pos = core * 4 + dq

    def issue_shared(part, s):
        cols = pl.ds(part * ff, ff)
        pltpu.make_async_copy(w1s.at[:, cols], slots.at[s, 0], wsem.at[s, 0]).start()
        pltpu.make_async_copy(w3s.at[:, cols], slots.at[s, 1], wsem.at[s, 1]).start()

    def issue_expert(e, s):
        pltpu.make_async_copy(w1e.at[e], slots.at[s, 0], wsem.at[s, 0]).start()
        pltpu.make_async_copy(w3e.at[e], slots.at[s, 1], wsem.at[s, 1]).start()

    def issue_down(c, s):
        cols = pl.ds(pl.multiple_of(c * CHUNK, CHUNK), CHUNK)
        for j in range(10):
            h, k = j // 5, j % 5
            src = w2e.at[j, :, cols] if j < experts else w2s.at[pl.ds((j - experts) * ff, ff), cols]
            dst = slots.at[s, h, pl.ds(0, ff), pl.ds(k * CHUNK, CHUNK)]
            pltpu.make_async_copy(src, dst, wsem.at[s, h]).start()

    def wait_full(s, h):
        pltpu.make_async_copy(w1e.at[0], slots.at[s, h], wsem.at[s, h]).wait()

    def wait_down(s, h):
        box = (pl.ds(0, ff), pl.ds(0, 5 * CHUNK))
        pltpu.make_async_copy(w1e.at[(0,) + box], slots.at[(s, h) + box], wsem.at[s, h]).wait()

    def up_project(lhs, s, dst, off):
        start = 0
        while start < ff:
            width = min(CHUNK, ff - start)
            cols = slice(start, start + width)
            gate = dot_f32(lhs[...], slots[s, 0, :, cols])
            lin = dot_f32(lhs[...], slots[s, 1, :, cols])
            dst[:, off + start:off + start + width] = (jax.nn.silu(gate) * lin).astype(BF16)
            start += width

    y_copy = pltpu.make_async_copy(y_hbm, y_ref, y_sem)
    y_copy.start()
    issue_shared(0, 0)
    issue_shared(1, 1)
    issue_expert(0, 2)

    barrier = pltpu.get_barrier_semaphore()
    for dev in (partner, xdev, ydev):
        pl.semaphore_signal(barrier, inc=1, device_id={"ep": dev}, device_id_type=pl.DeviceIdType.MESH)

    y_copy.wait()
    rows_f = y_ref[...].astype(F32)
    inv_rms = lax.rsqrt(jnp.mean(rows_f * rows_f, axis=-1, keepdims=True) + NORM_EPS)
    ball[my_pos] = (rows_f * inv_rms * gain_ref[...].astype(F32)).astype(BF16)
    pl.semaphore_wait(barrier, 3)

    def remote(t, src, dst, dev):
        return pltpu.make_async_remote_copy(
            src_ref=src, dst_ref=dst, send_sem=ssem.at[t], recv_sem=rsem.at[t],
            device_id={"ep": dev}, device_id_type=pl.DeviceIdType.MESH)

    def block(pos, h=None):
        return ball.at[pos] if h is None else ball.at[pos, pl.ds(h * half, half)]

    def same(t, ref, dev):
        return remote(t, ref, ref, dev)

    x_h0 = same(0, block(my_pos, 0), xdev)
    y_h1 = same(1, block(my_pos, 1), ydev)
    x_h1 = same(2, block(my_pos, 1), xdev)
    y_h0 = same(3, block(my_pos, 0), ydev)
    p_own = same(4, block(my_pos), partner)
    for cp in (x_h0, y_h1, x_h1, y_h0, p_own):
        cp.start()

    logits = lax.dot_general(wgt_ref[...], ball[my_pos], (((1,), (1,)), ((), ())), preferred_element_type=F32)
    expv = jnp.exp(logits - jnp.max(logits, axis=0, keepdims=True))
    probs = expv / jnp.sum(expv, axis=0, keepdims=True)
    eid = lax.broadcasted_iota(jnp.int32, logits.shape, 0)
    chosen = idst_ref[0:1, :] == eid
    for j in range(1, idst_ref.shape[0]):
        chosen = jnp.logical_or(chosen, idst_ref[j:j + 1, :] == eid)
    vall[my_pos] = jnp.full(vall.shape[1:], -1.0, F32)
    vall[my_pos, :, 0:rows] = jnp.where(chosen, ROUTE_SCALE * probs, -1.0)

    x_v = same(5, vall.at[my_pos], xdev)
    y_v = same(6, vall.at[my_pos], ydev)
    p_v = same(7, vall.at[my_pos], partner)
    for cp in (x_v, y_v, p_v):
        cp.start()

    wait_full(0, 0)
    wait_full(0, 1)
    up_project(ball.at[my_pos], 0, act_s, 0)
    issue_expert(1, 0)

    x_h0.wait_recv()
    f_h0 = same(8, block(x_pos, 0), ydev)
    f_h0.start()
    y_h1.wait_recv()
    f_h1 = same(9, block(y_pos, 1), xdev)
    f_h1.start()
    x_v.wait_recv()
    f_v = same(10, vall.at[x_pos], ydev)
    f_v.start()
    y_v.wait_recv()
    p_xv = same(11, vall.at[x_pos], partner)
    p_yv = same(12, vall.at[y_pos], partner)
    p_xv.start()
    p_yv.start()

    wait_full(1, 0)
    wait_full(1, 1)
    up_project(ball.at[my_pos], 1, act_s, ff)
    issue_expert(2, 1)

    upper = lax.broadcasted_iota(jnp.int32, (tokens, tokens), 0) < lax.broadcasted_iota(jnp.int32, (tokens, tokens), 1)
    upper = jnp.where(upper, 1.0, 0.0).astype(BF16)

    x_h1.wait_recv()
    p_x = same(13, block(x_pos), partner)
    p_x.start()
    y_h0.wait_recv()
    p_y = same(14, block(y_pos), partner)
    p_y.start()
    f_v.wait_recv()
    p_dv = same(15, vall.at[d_pos], partner)
    p_dv.start()
    f_h0.wait_recv()
    p_d0 = same(16, block(d_pos, 0), partner)
    p_d0.start()
    f_h1.wait_recv()
    p_d1 = same(17, block(d_pos, 1), partner)
    p_d1.start()
    for cp in (p_v, p_xv, p_yv, p_dv):
        cp.wait_recv()

    for k in range(8):
        vt_ref[:, k * rows:(k + 1) * rows] = vall[k, :, 0:rows]
    counts = jnp.sum(jnp.where(vt_ref[...] > -0.5, 1.0, 0.0), axis=1, keepdims=True)
    load_ref[...] = jnp.broadcast_to(jnp.max(counts, axis=0, keepdims=True), load_ref.shape)
    v_loc = vt_ref[pl.ds(pl.multiple_of(me * experts, experts), experts), :]
    sel = v_loc > -0.5
    picks = jnp.where(sel, 1.0, 0.0)
    picks = jnp.concatenate([picks, picks], axis=0).astype(BF16)
    rank = dot_f32(picks, upper)[0:experts] - base_ref[0:1, 0:1]
    rank = jnp.where(sel, rank, -1.0)
    rk_ref[...] = rank
    stacked = jnp.concatenate(
        [rank, jnp.where(sel, v_loc, 0.0), jnp.zeros((128 - 2 * experts, tokens), F32)], axis=0)
    tr_ref[...] = stacked.T
    lane = lax.broadcasted_iota(jnp.int32, (tokens, CAP), 1).astype(F32)
    for e in range(experts):
        q_all[e] = jnp.where(tr_ref[:, e:e + 1] == lane, 1.0, 0.0).astype(BF16)

    for cp in (p_own, p_x, p_y, p_d0, p_d1):
        cp.wait_recv()

    slot_row = lax.broadcasted_iota(jnp.int32, (CAP, tokens), 0).astype(F32)

    def stage_one(e, carry):
        s = (e + 2) % RING
        pick = jnp.where(rk_ref[pl.ds(e, 1), :] == slot_row, 1.0, 0.0).astype(BF16)
        for k in range(0, ball.shape[2], 512):
            xg_ref[:, k:k + 512] = dot_f32(pick, ball[:, :, k:k + 512].reshape(tokens, 512)).astype(BF16)
        wait_full(s, 0)
        wait_full(s, 1)
        up_project(xg_ref, s, act_ref.at[e], 0)

        @pl.when(e + RING < experts)
        def _():
            issue_expert(e + RING, s)

        @pl.when(e + RING >= experts)
        def _():
            issue_down(e + RING - experts, s)

        return carry

    lax.fori_loop(0, experts, stage_one, 0)

    def send_d(c):
        return pltpu.make_async_remote_copy(
            src_ref=pbuf.at[c, 1 - core], dst_ref=dbuf.at[c], send_sem=ds_sem.at[c], recv_sem=dr_sem.at[c],
            device_id={"ep": partner}, device_id_type=pl.DeviceIdType.MESH)

    def send_a(c, i):
        return pltpu.make_async_remote_copy(
            src_ref=pbuf.at[c, core, dq, pl.ds(i * half, half)], dst_ref=abuf.at[c, i],
            send_sem=as_sem.at[c, i], recv_sem=ar_sem.at[c, i],
            device_id={"ep": (xdev, ydev)[i]}, device_id_type=pl.DeviceIdType.MESH)

    def send_b(c, i):
        return pltpu.make_async_remote_copy(
            src_ref=pbuf.at[c, core, (xq, yq)[i]], dst_ref=rbuf.at[c, i],
            send_sem=bs_sem.at[c, i], recv_sem=br_sem.at[c, i],
            device_id={"ep": (xdev, ydev)[i]}, device_id_type=pl.DeviceIdType.MESH)

    def compute_chunk(c):
        s = (c + experts + 2) % RING
        wait_down(s, 0)
        wait_down(s, 1)
        total = None
        for e in range(experts):
            slab = slots[s, e // 5, 0:ff, (e % 5) * CHUNK:(e % 5 + 1) * CHUNK]
            res = dot_f32(act_ref[e], slab).astype(BF16)
            part = tr_ref[:, experts + e:experts + e + 1] * dot_f32(q_all[e], res)
            part = part.reshape(pbuf.shape[1:])
            if e == 0:
                pbuf[c] = part
            else:
                pbuf[c] = pbuf[c] + part
        lo = slots[s, 1, 0:ff, 3 * CHUNK:4 * CHUNK]
        hi = slots[s, 1, 0:ff, 4 * CHUNK:5 * CHUNK]
        sbuf[c] = (dot_f32(act_s[:, 0:ff], lo) + dot_f32(act_s[:, ff:2 * ff], hi)).astype(BF16)

        @pl.when(c + RING < chunks)
        def _():
            issue_down(c + RING, s)

        send_d(c).start()

    def reduce_pair(c):
        send_d(c).wait_recv()
        pbuf[c, core] = pbuf[c, core] + dbuf[c]
        send_a(c, 0).start()
        send_a(c, 1).start()

    def reduce_diag(c):
        send_a(c, 0).wait_recv()
        pbuf[c, core, yq, 0:half] = pbuf[c, core, yq, 0:half] + abuf[c, 0]
        send_b(c, 1).start()
        send_a(c, 1).wait_recv()
        pbuf[c, core, xq, half:rows] = pbuf[c, core, xq, half:rows] + abuf[c, 1]
        send_b(c, 0).start()

    def finish(c):
        cols = pl.ds(pl.multiple_of(c * CHUNK, CHUNK), CHUNK)
        local = y_ref[:, cols].astype(F32) + sbuf[c].astype(F32)
        local = jnp.where(base_ref[0:1, 0:1] == 0.0, local, 0.0)
        send_b(c, 0).wait_recv()
        send_b(c, 1).wait_recv()
        out_ref[:, cols] = local + (pbuf[c, core, chip] + rbuf[c, 0] + rbuf[c, 1])

    def stage_two(c, carry):
        pl.when(c < chunks)(lambda: compute_chunk(c))
        pl.when(jnp.logical_and(c >= 1, c < chunks + 1))(lambda: reduce_pair(c - 1))
        pl.when(jnp.logical_and(c >= 2, c < chunks + 2))(lambda: reduce_diag(c - 2))
        pl.when(c >= 3)(lambda: finish(c - 3))
        return carry

    lax.fori_loop(0, chunks + 3, stage_two, 0)

    for cp in (x_h0, y_h1, x_h1, y_h0, p_own, x_v, y_v, p_v, f_h0, f_h1, f_v, p_xv, p_yv, p_x, p_y, p_dv, p_d0, p_d1):
        cp.wait_send()

    def drain(c, carry):
        send_d(c).wait_send()
        for i in range(2):
            send_a(c, i).wait_send()
            send_b(c, i).wait_send()
        return carry

    lax.fori_loop(0, chunks, drain, 0)


def moe_call(base, gain, wgt, idst, y, w1s, w3s, w2s, w1e, w3e, w2e):
    rows, width = y.shape
    experts, _, ff = w1e.shape
    all_experts = wgt.shape[0]
    tokens = rows * 8
    chunks = width // CHUNK
    vmem = pl.BlockSpec(memory_space=pltpu.VMEM)
    hbm = pl.BlockSpec(memory_space=pl.ANY)
    dma = pltpu.SemaphoreType.DMA
    return pl.pallas_call(
        moe_kernel,
        out_shape=(jax.ShapeDtypeStruct((rows, width), F32), jax.ShapeDtypeStruct((8, 128), F32)),
        in_specs=[vmem] * 4 + [hbm] * 7,
        out_specs=(vmem, vmem),
        scratch_shapes=[
            pltpu.VMEM((rows, width), BF16),
            pltpu.VMEM((RING, 2, width, ff), BF16),
            pltpu.VMEM((8, rows, width), BF16),
            pltpu.VMEM((8, all_experts, 128), F32),
            pltpu.VMEM((all_experts, tokens), F32),
            pltpu.VMEM((experts, tokens), F32),
            pltpu.VMEM((tokens, 128), F32),
            pltpu.VMEM((experts, tokens, CAP), BF16),
            pltpu.VMEM((CAP, width), BF16),
            pltpu.VMEM((experts, CAP, ff), BF16),
            pltpu.VMEM((rows, 2 * ff), BF16),
            pltpu.VMEM((chunks, 2, 4, rows, CHUNK), F32),
            pltpu.VMEM((chunks, 4, rows, CHUNK), F32),
            pltpu.VMEM((chunks, 2, rows // 2, CHUNK), F32),
            pltpu.VMEM((chunks, 2, rows, CHUNK), F32),
            pltpu.VMEM((chunks, rows, CHUNK), BF16),
            dma,
            dma((RING, 2)),
            dma((18,)),
            dma((18,)),
            dma((chunks,)),
            dma((chunks,)),
            dma((chunks, 2)),
            dma((chunks, 2)),
            dma((chunks, 2)),
            dma((chunks, 2)),
        ],
        compiler_params=pltpu.CompilerParams(
            collective_id=0, has_side_effects=True, vmem_limit_bytes=67_000_000),
    )(base, gain, wgt, idst, y, w1s, w3s, w2s, w1e, w3e, w2e)


def solution(mesh):
    tok_spec = P(('dp', 'ep'), None)
    expert_spec = P('ep', None, None)

    def local_fn(hidden, norm_gain, w_gate, w1_shared, w3_shared, w2_shared, w1_experts, w3_experts, w2_experts, topk_ids):
        def routed_round(base):
            return moe_call(base, norm_gain[None, :], w_gate.T, topk_ids.T, hidden, w1_shared, w3_shared, w2_shared,
                            w1_experts, w3_experts, w2_experts)

        total, load = routed_round(jnp.zeros((8, 128), F32))

        def more(state):
            return state[0] < load[0, 0]

        def body(state):
            start, acc = state
            part, _ = routed_round(jnp.full((8, 128), start, F32))
            return start + CAP, acc + part

        total = lax.while_loop(more, body, (jnp.float32(CAP), total))[1]
        return total.astype(BF16)

    return jax.shard_map(local_fn, mesh=mesh, in_specs=(tok_spec, P(), P(), P(), P(), P(), expert_spec, expert_spec, expert_spec, tok_spec), out_specs=tok_spec, check_vma=False)
```

```python
import functools

import jax
import jax.numpy as jnp
from jax import lax
from jax.experimental import pallas as pl
from jax.experimental.pallas import tpu as pltpu
from jax.sharding import PartitionSpec as P

ROUTE_SCALE = 16
NORM_EPS = 1e-6
CAP = 128
CHUNK = 256
RING = 4
WIDE = 512
F32 = jnp.float32
BF16 = jnp.bfloat16


def dot_f32(lhs, rhs):
    return jnp.dot(lhs, rhs, preferred_element_type=F32)


def moe_kernel(first, *refs):
    if first:
        base = 0.0
    else:
        base, refs = refs[0][0:1, 0:1], refs[1:]
    (gain_ref, wgt_ref, idst_ref, y_ref, w1s, w3s, w2s, w1e, w3e, w2e,
     out_hbm, load_hbm,
     out_ref, load_ref, slots, ball, vall, vt_ref, rk_ref, tr_ref, q_all, xg_ref, act_ref, act_s,
     pbuf, obuf, dbuf, abuf, rbuf, s_ref, e_ref,
     out_sem, load_sem, wsem, ssem, rsem, ds_sem, dr_sem, as_sem, ar_sem, bs_sem, br_sem) = refs
    rows = y_ref.shape[0]
    half = rows // 2
    experts, _, ff = w1e.shape
    picks_per_row = idst_ref.shape[0]
    chunks = w2e.shape[2] // CHUNK
    tokens = rows * 8
    me = lax.axis_index("ep")
    core = me % 2
    chip = me // 2
    xpos = chip % 2
    ypos = chip // 2
    partner = me + 1 - 2 * core
    xdev = me + 2 - 4 * xpos
    ydev = me + 4 - 8 * ypos
    xq = chip + 1 - 2 * xpos
    yq = chip + 2 - 4 * ypos
    dq = 3 - chip
    diag = 2 * dq + core

    def issue_shared(part, s):
        cols = pl.ds(part * ff, ff)
        pltpu.make_async_copy(w1s.at[:, cols], slots.at[s, 0], wsem.at[s, 0]).start()
        pltpu.make_async_copy(w3s.at[:, cols], slots.at[s, 1], wsem.at[s, 1]).start()

    def issue_expert(e, s):
        pltpu.make_async_copy(w1e.at[e], slots.at[s, 0], wsem.at[s, 0]).start()
        pltpu.make_async_copy(w3e.at[e], slots.at[s, 1], wsem.at[s, 1]).start()

    def issue_down(c, s):
        cols = pl.ds(pl.multiple_of(c * CHUNK, CHUNK), CHUNK)
        for j in range(experts + 2):
            h, k = j // 5, j % 5
            src = w2e.at[j, :, cols] if j < experts else w2s.at[pl.ds((j - experts) * ff, ff), cols]
            dst = slots.at[s, h, pl.ds(0, ff), pl.ds(k * CHUNK, CHUNK)]
            pltpu.make_async_copy(src, dst, wsem.at[s, h]).start()

    def wait_full(s, h):
        pltpu.make_async_copy(w1e.at[0], slots.at[s, h], wsem.at[s, h]).wait()

    def wait_down(s, h):
        box = (pl.ds(0, ff), pl.ds(0, 5 * CHUNK))
        pltpu.make_async_copy(w1e.at[(0,) + box], slots.at[(s, h) + box], wsem.at[s, h]).wait()

    def up_project(lhs, s, dst, off):
        body = ff // CHUNK * CHUNK
        rest = ff - body
        for start in range(0, body, CHUNK):
            cols = slice(start, start + CHUNK)
            gate = dot_f32(lhs[...], slots[s, 0, :, cols])
            lin = dot_f32(lhs[...], slots[s, 1, :, cols])
            dst[:, off + start:off + start + CHUNK] = (jax.nn.silu(gate) * lin).astype(BF16)
        both = jnp.concatenate([slots[s, 0, :, body:ff], slots[s, 1, :, body:ff]], axis=1)
        both = dot_f32(lhs[...], both)
        dst[:, off + body:off + ff] = (jax.nn.silu(both[:, 0:rest]) * both[:, rest:]).astype(BF16)

    barrier = pltpu.get_barrier_semaphore()
    for dev in (partner, xdev, ydev, diag):
        pl.semaphore_signal(barrier, inc=1, device_id={"ep": dev}, device_id_type=pl.DeviceIdType.MESH)
    issue_shared(0, 0)
    issue_shared(1, 1)
    issue_expert(0, 2)
    issue_expert(1, 3)

    rows_f = y_ref[...].astype(F32)
    inv_rms = lax.rsqrt(jnp.mean(rows_f * rows_f, axis=-1, keepdims=True) + NORM_EPS)
    ball[me] = (rows_f * inv_rms * gain_ref[...].astype(F32).reshape(1, y_ref.shape[1])).astype(BF16)
    logits = lax.dot_general(wgt_ref[...], ball[me], (((1,), (1,)), ((), ())), preferred_element_type=F32)
    expv = jnp.exp(logits - jnp.max(logits, axis=0, keepdims=True))
    probs = expv / jnp.sum(expv, axis=0, keepdims=True)
    eid = lax.broadcasted_iota(jnp.int32, logits.shape, 0)
    vall[me] = jnp.full(vall.shape[1:], -1.0, F32)
    for j in range(picks_per_row):
        ids = idst_ref[j:j + 1, :]
        vall[me, j:j + 1, 0:rows] = ids.astype(F32)
        weight = jnp.sum(jnp.where(ids == eid, probs, 0.0), axis=0, keepdims=True)
        vall[me, 8 + j:9 + j, 0:rows] = ROUTE_SCALE * weight
    pl.semaphore_wait(barrier, 4)

    def same(t, ref, dev):
        return pltpu.make_async_remote_copy(
            src_ref=ref, dst_ref=ref, send_sem=ssem.at[t], recv_sem=rsem.at[t],
            device_id={"ep": dev}, device_id_type=pl.DeviceIdType.MESH)

    def block(dev, h=None):
        return ball.at[dev] if h is None else ball.at[dev, pl.ds(h * half, half)]

    x_v = same(0, vall.at[me], xdev)
    y_v = same(1, vall.at[me], ydev)
    p_v = same(2, vall.at[me], partner)
    d_v = same(8, vall.at[me], diag)
    x_h0 = same(3, block(me, 0), xdev)
    y_h1 = same(4, block(me, 1), ydev)
    x_h1 = same(5, block(me, 1), xdev)
    y_h0 = same(6, block(me, 0), ydev)
    p_own = same(7, block(me), partner)
    for cp in (x_v, y_v, d_v, p_v, x_h0, y_h1, x_h1, y_h0, p_own):
        cp.start()
    p_xv = same(9, vall.at[xdev], partner)
    p_yv = same(10, vall.at[ydev], partner)
    p_dv = same(11, vall.at[diag], partner)
    f_h0 = same(12, block(xdev, 0), ydev)
    f_h1 = same(13, block(ydev, 1), xdev)
    p_x = same(14, block(xdev), partner)
    p_y = same(15, block(ydev), partner)
    p_d0 = same(16, block(diag, 0), partner)
    p_d1 = same(17, block(diag, 1), partner)

    wait_full(0, 0)
    wait_full(0, 1)
    up_project(ball.at[me], 0, act_s, 0)
    issue_expert(2, 0)
    x_v.wait_recv()
    p_xv.start()
    y_v.wait_recv()
    p_yv.start()
    d_v.wait_recv()
    p_dv.start()
    x_h0.wait_recv()
    f_h0.start()
    y_h1.wait_recv()
    f_h1.start()

    wait_full(1, 0)
    wait_full(1, 1)
    up_project(ball.at[me], 1, act_s, ff)
    issue_expert(3, 1)
    for cp in (p_v, p_xv, p_yv, p_dv):
        cp.wait_recv()

    for k in range(8):
        vt_ref[:, k * rows:(k + 1) * rows] = vall[k, :, 0:rows]
    all_experts = wgt_ref.shape[0]
    every = lax.broadcasted_iota(jnp.int32, (all_experts, tokens), 0).astype(F32)
    hits = jnp.zeros((all_experts, tokens), F32)
    for j in range(picks_per_row):
        hits = hits + jnp.where(vt_ref[j:j + 1, :] == every, 1.0, 0.0)
    load_ref[0, 0] = jnp.max(jnp.sum(hits, axis=1, keepdims=True))
    load_copy = pltpu.make_async_copy(load_ref, load_hbm, load_sem)
    load_copy.start()
    local = (lax.broadcasted_iota(jnp.int32, (experts, tokens), 0) + me * experts).astype(F32)
    picks = jnp.zeros((experts, tokens), F32)
    weights = jnp.zeros((experts, tokens), F32)
    for j in range(picks_per_row):
        match = vt_ref[j:j + 1, :] == local
        picks = jnp.where(match, 1.0, picks)
        weights = jnp.where(match, vt_ref[8 + j:9 + j, :], weights)
    sel = picks > 0.5
    picks = jnp.concatenate([picks, picks], axis=0).astype(BF16)
    upper = lax.broadcasted_iota(jnp.int32, (tokens, tokens), 0) < lax.broadcasted_iota(jnp.int32, (tokens, tokens), 1)
    upper = jnp.where(upper, 1.0, 0.0).astype(BF16)
    rank = dot_f32(picks, upper)[0:experts] - base
    rank = jnp.where(sel, rank, -1.0)
    rk_ref[0:experts, :] = rank
    rk_ref[experts:2 * experts, :] = weights

    x_h1.wait_recv()
    p_x.start()
    y_h0.wait_recv()
    p_y.start()

    stacked = jnp.concatenate([rk_ref[...], jnp.zeros((128 - 2 * experts, tokens), F32)], axis=0).T
    for k in range(8):
        pos = (k % 2) * 4 + k // 2
        tr_ref[pos * rows:(pos + 1) * rows, :] = stacked[k * rows:(k + 1) * rows, :]
    lane = lax.broadcasted_iota(jnp.int32, (tokens, CAP), 1).astype(F32)
    for e in range(experts):
        q_all[e] = jnp.where(tr_ref[:, e:e + 1] == lane, 1.0, 0.0).astype(BF16)

    f_h0.wait_recv()
    p_d0.start()
    f_h1.wait_recv()
    p_d1.start()
    for cp in (p_own, p_x, p_y, p_d0, p_d1):
        cp.wait_recv()

    slot_row = lax.broadcasted_iota(jnp.int32, (CAP, tokens), 0).astype(F32)
    width = ball.shape[2]

    def stage_one(e, carry):
        s = (e + 2) % RING
        pick = jnp.where(rk_ref[pl.ds(e, 1), :] == slot_row, 1.0, 0.0).astype(BF16)
        for k in range(0, width, WIDE):
            xg_ref[:, k:k + WIDE] = dot_f32(pick, ball[:, :, k:k + WIDE].reshape(tokens, WIDE)).astype(BF16)
        wait_full(s, 0)
        wait_full(s, 1)
        up_project(xg_ref, s, act_ref.at[e], 0)

        @pl.when(e + RING < experts)
        def _():
            issue_expert(e + RING, s)

        @pl.when(e + RING >= experts)
        def _():
            issue_down(e + RING - experts, s)

        return carry

    lax.fori_loop(0, experts, stage_one, 0)

    for cp in (x_v, y_v, d_v, p_v, x_h0, y_h1, x_h1, y_h0, p_own, p_xv, p_yv, p_dv, f_h0, f_h1, p_x, p_y, p_d0, p_d1):
        cp.wait_send()

    load_copy.wait()

    def send_d(c):
        return pltpu.make_async_remote_copy(
            src_ref=obuf.at[c % 2], dst_ref=dbuf.at[c % 2], send_sem=ds_sem.at[c], recv_sem=dr_sem.at[c],
            device_id={"ep": partner}, device_id_type=pl.DeviceIdType.MESH)

    def send_a(c, i):
        return pltpu.make_async_remote_copy(
            src_ref=pbuf.at[c, dq, pl.ds(i * half, half)], dst_ref=abuf.at[c, i],
            send_sem=as_sem.at[c, i], recv_sem=ar_sem.at[c, i],
            device_id={"ep": (xdev, ydev)[i]}, device_id_type=pl.DeviceIdType.MESH)

    def send_b(c, i, h):
        return pltpu.make_async_remote_copy(
            src_ref=pbuf.at[c, (xq, yq)[i], pl.ds(h * half, half)], dst_ref=rbuf.at[c, i, h],
            send_sem=bs_sem.at[c, i, h], recv_sem=br_sem.at[c, i, h],
            device_id={"ep": (xdev, ydev)[i]}, device_id_type=pl.DeviceIdType.MESH)

    def out_copy(c):
        cols = pl.ds(pl.multiple_of(c * CHUNK, CHUNK), CHUNK)
        return pltpu.make_async_copy(out_ref.at[:, cols], out_hbm.at[:, cols], out_sem.at[c])

    def down_project(c):
        s = (c + experts + 2) % RING
        wait_down(s, 0)
        wait_down(s, 1)
        for e in range(experts):
            slab = slots[s, e // 5, 0:ff, (e % 5) * CHUNK:(e % 5 + 1) * CHUNK]
            e_ref[e] = dot_f32(act_ref[e], slab).astype(BF16)
        lo = slots[s, 1, 0:ff, 3 * CHUNK:4 * CHUNK]
        hi = slots[s, 1, 0:ff, 4 * CHUNK:5 * CHUNK]
        cols = pl.ds(pl.multiple_of(c * CHUNK, CHUNK), CHUNK)
        s_ref[:, cols] = (dot_f32(act_s[:, 0:ff], lo) + dot_f32(act_s[:, ff:2 * ff], hi)).astype(BF16)

        @pl.when(c + RING < chunks)
        def _():
            issue_down(c + RING, s)

    def combine_side(dst, slot, side):
        own = pl.ds(pl.multiple_of(side * (tokens // 2), tokens // 2), tokens // 2)
        for e in range(experts):
            part = tr_ref[own, experts + e:experts + e + 1] * dot_f32(q_all[e, own, :], e_ref[e])
            part = part.reshape(dst.shape[1:])
            if e == 0:
                dst[slot] = part
            else:
                dst[slot] = dst[slot] + part

    def combine(c):
        @pl.when(c >= 2)
        def _():
            send_d(c - 2).wait_send()

        combine_side(obuf, c % 2, 1 - core)
        send_d(c).start()
        combine_side(pbuf, c, core)

    def reduce_pair(c):
        send_d(c).wait_recv()
        pbuf[c] = pbuf[c] + dbuf[c % 2]
        for i in range(2):
            send_a(c, i).start()
        for i in range(2):
            send_b(c, i, i).start()

    def reduce_diag(c):
        for i in range(2):
            send_a(c, 1 - i).wait_recv()
            q = (xq, yq)[i]
            rest = slice((1 - i) * half, (2 - i) * half)
            pbuf[c, q, rest] = pbuf[c, q, rest] + abuf[c, 1 - i]
            send_b(c, i, 1 - i).start()

    def finish(c):
        cols = pl.ds(pl.multiple_of(c * CHUNK, CHUNK), CHUNK)
        local = y_ref[:, cols].astype(F32) + s_ref[:, cols].astype(F32)
        if not first:
            local = jnp.where(base == 0.0, local, 0.0)
        for h in range(2):
            part = slice(h * half, (h + 1) * half)
            routed = pbuf[c, chip, part]
            for i in range(2):
                send_b(c, i, h).wait_recv()
                routed = routed + rbuf[c, i, h]
            out_ref[part, cols] = (local[part] + routed).astype(out_ref.dtype)
        out_copy(c).start()

        @pl.when(c >= chunks - 2)
        def _():
            send_d(c).wait_send()

        for i in range(2):
            send_a(c, i).wait_send()
            for h in range(2):
                send_b(c, i, h).wait_send()

    def stage_two(c, carry):
        pl.when(c < chunks)(lambda: down_project(c))
        pl.when(jnp.logical_and(c >= 1, c < chunks + 1))(lambda: reduce_pair(c - 1))
        pl.when(c < chunks)(lambda: combine(c))
        pl.when(jnp.logical_and(c >= 2, c < chunks + 2))(lambda: reduce_diag(c - 2))
        pl.when(c >= 4)(lambda: finish(c - 4))
        return carry

    lax.fori_loop(0, chunks + 4, stage_two, 0)

    def drain(c, carry):
        out_copy(c).wait()
        return carry

    lax.fori_loop(0, chunks, drain, 0)


def moe_call(base, gain, wgt, idst, y, w1s, w3s, w2s, w1e, w3e, w2e):
    first = base is None
    rows, width = y.shape
    experts, _, ff = w1e.shape
    tokens = rows * 8
    chunks = width // CHUNK
    vmem = pl.BlockSpec(memory_space=pltpu.VMEM)
    hbm = pl.BlockSpec(memory_space=pl.ANY)
    dma = pltpu.SemaphoreType.DMA
    small = ([] if first else [base]) + [gain, wgt, idst]
    return pl.pallas_call(
        functools.partial(moe_kernel, first),
        out_shape=(jax.ShapeDtypeStruct((rows, width), BF16 if first else F32), jax.ShapeDtypeStruct((1, 1), F32)),
        in_specs=[vmem] * (len(small) + 1) + [hbm] * 6,
        out_specs=(hbm, hbm),
        scratch_shapes=[
            pltpu.VMEM((rows, width), BF16 if first else F32),
            pltpu.SMEM((1, 1), F32),
            pltpu.VMEM((RING, 2, width, ff), BF16),
            pltpu.VMEM((8, rows, width), BF16),
            pltpu.VMEM((8, 16, 128), F32),
            pltpu.VMEM((16, tokens), F32),
            pltpu.VMEM((2 * experts, tokens), F32),
            pltpu.VMEM((tokens, 128), F32),
            pltpu.VMEM((experts, tokens, CAP), BF16),
            pltpu.VMEM((CAP, width), BF16),
            pltpu.VMEM((experts, CAP, ff), BF16),
            pltpu.VMEM((rows, 2 * ff), BF16),
            pltpu.VMEM((chunks, 4, rows, CHUNK), F32),
            pltpu.VMEM((2, 4, rows, CHUNK), F32),
            pltpu.VMEM((2, 4, rows, CHUNK), F32),
            pltpu.VMEM((chunks, 2, rows // 2, CHUNK), F32),
            pltpu.VMEM((chunks, 2, 2, rows // 2, CHUNK), F32),
            pltpu.VMEM((rows, width), BF16),
            pltpu.VMEM((experts, CAP, CHUNK), BF16),
            dma((chunks,)),
            dma,
            dma((RING, 2)),
            dma((18,)),
            dma((18,)),
            dma((chunks,)),
            dma((chunks,)),
            dma((chunks, 2)),
            dma((chunks, 2)),
            dma((chunks, 2, 2)),
            dma((chunks, 2, 2)),
        ],
        compiler_params=pltpu.CompilerParams(
            collective_id=0 if first else 1, has_side_effects=True, vmem_limit_bytes=67_000_000),
    )(*small, y, w1s, w3s, w2s, w1e, w3e, w2e)


def solution(mesh):
    tok_spec = P(('dp', 'ep'), None)
    expert_spec = P('ep', None, None)

    def local_fn(hidden, norm_gain, w_gate, w1_shared, w3_shared, w2_shared, w1_experts, w3_experts, w2_experts, topk_ids):
        def routed_round(base):
            return moe_call(base, norm_gain, w_gate.T, topk_ids.T, hidden, w1_shared, w3_shared, w2_shared,
                            w1_experts, w3_experts, w2_experts)

        out, load = routed_round(None)

        def overflow(state):
            def add_round(i, acc):
                return acc + routed_round(jnp.full((8, 128), i * CAP, F32))[0]

            rounds = jnp.ceil(state[0] / CAP).astype(jnp.int32)
            acc = lax.fori_loop(0, rounds, add_round, jnp.zeros(hidden.shape, F32))
            return jnp.float32(0), acc.astype(BF16)

        return lax.while_loop(lambda state: state[0] > CAP, overflow, (load[0, 0], out))[1]

    return jax.shard_map(local_fn, mesh=mesh, in_specs=(tok_spec, P(), P(), P(), P(), P(), expert_spec, expert_spec, expert_spec, tok_spec), out_specs=tok_spec, check_vma=False)
```

```python
import functools

import jax
import jax.numpy as jnp
from jax import lax
from jax.experimental import pallas as pl
from jax.experimental.pallas import tpu as pltpu
from jax.sharding import PartitionSpec as P

ROUTE_SCALE = 16
NORM_EPS = 1e-6
CAP = 128
CHUNK = 256
RING = 4
WIDE = 512
F32 = jnp.float32
BF16 = jnp.bfloat16


def dot_f32(lhs, rhs):
    return jnp.dot(lhs, rhs, preferred_element_type=F32)


def moe_kernel(first, *refs):
    if first:
        base = 0.0
    else:
        base, refs = refs[0][0:1, 0:1], refs[1:]
    (gain_ref, wgt_ref, idst_ref, y_ref, w1s, w3s, w2s, w1e, w3e, w2e,
     out_hbm, load_hbm,
     out_ref, load_ref, slots, ball, vall, vt_ref, rk_ref, tr_ref, q_all, xg_ref, act_ref, act_s,
     pbuf, obuf, dbuf, abuf, rbuf, s_ref, e_ref,
     out_sem, load_sem, wsem, ssem, rsem, ds_sem, dr_sem, as_sem, ar_sem, bs_sem, br_sem) = refs
    rows = y_ref.shape[0]
    half = rows // 2
    experts, _, ff = w1e.shape
    picks_per_row = idst_ref.shape[0]
    chunks = w2e.shape[2] // CHUNK
    tokens = rows * 8
    me = lax.axis_index("ep")
    core = me % 2
    chip = me // 2
    xpos = chip % 2
    ypos = chip // 2
    partner = me + 1 - 2 * core
    xdev = me + 2 - 4 * xpos
    ydev = me + 4 - 8 * ypos
    xq = chip + 1 - 2 * xpos
    yq = chip + 2 - 4 * ypos
    dq = 3 - chip
    diag = 2 * dq + core

    def issue_shared(part, s):
        cols = pl.ds(part * ff, ff)
        pltpu.make_async_copy(w1s.at[:, cols], slots.at[s, 0], wsem.at[s, 0]).start()
        pltpu.make_async_copy(w3s.at[:, cols], slots.at[s, 1], wsem.at[s, 1]).start()

    def issue_expert(e, s):
        pltpu.make_async_copy(w1e.at[e], slots.at[s, 0], wsem.at[s, 0]).start()
        pltpu.make_async_copy(w3e.at[e], slots.at[s, 1], wsem.at[s, 1]).start()

    def issue_down(c, s):
        cols = pl.ds(pl.multiple_of(c * CHUNK, CHUNK), CHUNK)
        for j in range(experts + 2):
            h, k = j // 5, j % 5
            src = w2e.at[j, :, cols] if j < experts else w2s.at[pl.ds((j - experts) * ff, ff), cols]
            dst = slots.at[s, h, pl.ds(0, ff), pl.ds(k * CHUNK, CHUNK)]
            pltpu.make_async_copy(src, dst, wsem.at[s, h]).start()

    def wait_full(s, h):
        pltpu.make_async_copy(w1e.at[0], slots.at[s, h], wsem.at[s, h]).wait()

    def wait_down(s, h):
        box = (pl.ds(0, ff), pl.ds(0, 5 * CHUNK))
        pltpu.make_async_copy(w1e.at[(0,) + box], slots.at[(s, h) + box], wsem.at[s, h]).wait()

    def up_project(lhs, s, dst, off):
        body = ff // CHUNK * CHUNK
        rest = ff - body
        for start in range(0, body, CHUNK):
            cols = slice(start, start + CHUNK)
            gate = dot_f32(lhs[...], slots[s, 0, :, cols])
            lin = dot_f32(lhs[...], slots[s, 1, :, cols])
            dst[:, off + start:off + start + CHUNK] = (jax.nn.silu(gate) * lin).astype(BF16)
        both = jnp.concatenate([slots[s, 0, :, body:ff], slots[s, 1, :, body:ff]], axis=1)
        both = dot_f32(lhs[...], both)
        dst[:, off + body:off + ff] = (jax.nn.silu(both[:, 0:rest]) * both[:, rest:]).astype(BF16)

    barrier = pltpu.get_barrier_semaphore()
    for dev in (partner, xdev, ydev, diag):
        pl.semaphore_signal(barrier, inc=1, device_id={"ep": dev}, device_id_type=pl.DeviceIdType.MESH)
    issue_shared(0, 0)
    issue_shared(1, 1)
    issue_expert(0, 2)
    issue_expert(1, 3)

    rows_f = y_ref[...].astype(F32)
    inv_rms = lax.rsqrt(jnp.mean(rows_f * rows_f, axis=-1, keepdims=True) + NORM_EPS)
    ball[me] = (rows_f * inv_rms * gain_ref[...].astype(F32).reshape(1, y_ref.shape[1])).astype(BF16)
    logits = lax.dot_general(wgt_ref[...], ball[me], (((1,), (1,)), ((), ())), preferred_element_type=F32)
    expv = jnp.exp(logits - jnp.max(logits, axis=0, keepdims=True))
    probs = expv / jnp.sum(expv, axis=0, keepdims=True)
    eid = lax.broadcasted_iota(jnp.int32, logits.shape, 0)
    vall[me] = jnp.full(vall.shape[1:], -1.0, F32)
    for j in range(picks_per_row):
        ids = idst_ref[j:j + 1, :]
        vall[me, j:j + 1, 0:rows] = ids.astype(F32)
        weight = jnp.sum(jnp.where(ids == eid, probs, 0.0), axis=0, keepdims=True)
        vall[me, 8 + j:9 + j, 0:rows] = ROUTE_SCALE * weight
    pl.semaphore_wait(barrier, 4)

    def same(t, ref, dev):
        return pltpu.make_async_remote_copy(
            src_ref=ref, dst_ref=ref, send_sem=ssem.at[t], recv_sem=rsem.at[t],
            device_id={"ep": dev}, device_id_type=pl.DeviceIdType.MESH)

    def block(dev, h=None):
        return ball.at[dev] if h is None else ball.at[dev, pl.ds(h * half, half)]

    x_v = same(0, vall.at[me], xdev)
    y_v = same(1, vall.at[me], ydev)
    p_v = same(2, vall.at[me], partner)
    d_v = same(8, vall.at[me], diag)
    x_h0 = same(3, block(me, 0), xdev)
    y_h1 = same(4, block(me, 1), ydev)
    x_h1 = same(5, block(me, 1), xdev)
    y_h0 = same(6, block(me, 0), ydev)
    p_own = same(7, block(me), partner)
    for cp in (x_v, y_v, d_v, p_v, x_h0, y_h1, x_h1, y_h0, p_own):
        cp.start()
    p_xv = same(9, vall.at[xdev], partner)
    p_yv = same(10, vall.at[ydev], partner)
    p_dv = same(11, vall.at[diag], partner)
    f_h0 = same(12, block(xdev, 0), ydev)
    f_h1 = same(13, block(ydev, 1), xdev)
    p_x = same(14, block(xdev), partner)
    p_y = same(15, block(ydev), partner)
    p_d0 = same(16, block(diag, 0), partner)
    p_d1 = same(17, block(diag, 1), partner)

    wait_full(0, 0)
    wait_full(0, 1)
    up_project(ball.at[me], 0, act_s, 0)
    issue_expert(2, 0)
    x_v.wait_recv()
    p_xv.start()
    y_v.wait_recv()
    p_yv.start()
    d_v.wait_recv()
    p_dv.start()
    x_h0.wait_recv()
    f_h0.start()
    y_h1.wait_recv()
    f_h1.start()

    wait_full(1, 0)
    wait_full(1, 1)
    up_project(ball.at[me], 1, act_s, ff)
    issue_expert(3, 1)
    for cp in (p_v, p_xv, p_yv, p_dv):
        cp.wait_recv()

    for k in range(8):
        vt_ref[:, k * rows:(k + 1) * rows] = vall[k, :, 0:rows]
    all_experts = wgt_ref.shape[0]
    every = lax.broadcasted_iota(jnp.int32, (all_experts, tokens), 0).astype(F32)
    hits = jnp.zeros((all_experts, tokens), F32)
    for j in range(picks_per_row):
        hits = hits + jnp.where(vt_ref[j:j + 1, :] == every, 1.0, 0.0)
    load_ref[0, 0] = jnp.max(jnp.sum(hits, axis=1, keepdims=True))
    load_copy = pltpu.make_async_copy(load_ref, load_hbm, load_sem)
    load_copy.start()
    local = (lax.broadcasted_iota(jnp.int32, (experts, tokens), 0) + me * experts).astype(F32)
    picks = jnp.zeros((experts, tokens), F32)
    weights = jnp.zeros((experts, tokens), F32)
    for j in range(picks_per_row):
        match = vt_ref[j:j + 1, :] == local
        picks = jnp.where(match, 1.0, picks)
        weights = jnp.where(match, vt_ref[8 + j:9 + j, :], weights)
    sel = picks > 0.5
    picks = jnp.concatenate([picks, picks], axis=0).astype(BF16)
    upper = lax.broadcasted_iota(jnp.int32, (tokens, tokens), 0) < lax.broadcasted_iota(jnp.int32, (tokens, tokens), 1)
    upper = jnp.where(upper, 1.0, 0.0).astype(BF16)
    rank = dot_f32(picks, upper)[0:experts] - base
    rank = jnp.where(sel, rank, -1.0)
    rk_ref[0:experts, :] = rank
    rk_ref[experts:2 * experts, :] = weights

    x_h1.wait_recv()
    p_x.start()
    y_h0.wait_recv()
    p_y.start()

    stacked = jnp.concatenate([rk_ref[...], jnp.zeros((128 - 2 * experts, tokens), F32)], axis=0).T
    for k in range(8):
        pos = (k % 2) * 4 + k // 2
        tr_ref[pos * rows:(pos + 1) * rows, :] = stacked[k * rows:(k + 1) * rows, :]
    lane = lax.broadcasted_iota(jnp.int32, (tokens, CAP), 1).astype(F32)
    for e in range(experts):
        q_all[e] = jnp.where(tr_ref[:, e:e + 1] == lane, 1.0, 0.0).astype(BF16)

    f_h0.wait_recv()
    p_d0.start()
    f_h1.wait_recv()
    p_d1.start()
    for cp in (p_own, p_x, p_y, p_d0, p_d1):
        cp.wait_recv()

    slot_row = lax.broadcasted_iota(jnp.int32, (CAP, tokens), 0).astype(F32)
    width = ball.shape[2]

    def gather(e):
        pick = jnp.where(rk_ref[pl.ds(e, 1), :] == slot_row, 1.0, 0.0).astype(BF16)
        for k in range(0, width, WIDE):
            xg_ref[e % 2, :, k:k + WIDE] = dot_f32(pick, ball[:, :, k:k + WIDE].reshape(tokens, WIDE)).astype(BF16)

    def stage_one(e, carry):
        s = (e + 2) % RING
        wait_full(s, 0)
        wait_full(s, 1)
        up_project(xg_ref.at[e % 2], s, act_ref.at[e], 0)
        gather(e + 1)

        @pl.when(e + RING < experts)
        def _():
            issue_expert(e + RING, s)

        @pl.when(e + RING >= experts)
        def _():
            issue_down(e + RING - experts, s)

        return carry

    gather(0)
    lax.fori_loop(0, experts, stage_one, 0)

    for cp in (x_v, y_v, d_v, p_v, x_h0, y_h1, x_h1, y_h0, p_own, p_xv, p_yv, p_dv, f_h0, f_h1, p_x, p_y, p_d0, p_d1):
        cp.wait_send()

    load_copy.wait()

    def send_d(c):
        return pltpu.make_async_remote_copy(
            src_ref=obuf.at[c % 2], dst_ref=dbuf.at[c % 2], send_sem=ds_sem.at[c % 2], recv_sem=dr_sem.at[c % 2],
            device_id={"ep": partner}, device_id_type=pl.DeviceIdType.MESH)

    def send_a(c, i):
        return pltpu.make_async_remote_copy(
            src_ref=pbuf.at[c, dq, pl.ds(i * half, half)], dst_ref=abuf.at[c, i],
            send_sem=as_sem.at[c % 4, i], recv_sem=ar_sem.at[c % 4, i],
            device_id={"ep": (xdev, ydev)[i]}, device_id_type=pl.DeviceIdType.MESH)

    def send_b(c, i, h=None):
        own = pl.ds(0, rows) if h is None else pl.ds(h * half, half)
        return pltpu.make_async_remote_copy(
            src_ref=pbuf.at[c, (xq, yq)[i], own], dst_ref=rbuf.at[c, i, own],
            send_sem=bs_sem.at[c % 4, i], recv_sem=br_sem.at[c, i],
            device_id={"ep": (xdev, ydev)[i]}, device_id_type=pl.DeviceIdType.MESH)

    def out_copy(c):
        cols = pl.ds(pl.multiple_of(c * CHUNK, CHUNK), CHUNK)
        return pltpu.make_async_copy(out_ref.at[:, cols], out_hbm.at[:, cols], out_sem.at[c % 2])

    def down_project(c):
        s = (c + experts + 2) % RING
        wait_down(s, 0)
        wait_down(s, 1)
        for e in range(experts):
            slab = slots[s, e // 5, 0:ff, (e % 5) * CHUNK:(e % 5 + 1) * CHUNK]
            e_ref[e] = dot_f32(act_ref[e], slab).astype(BF16)
        lo = slots[s, 1, 0:ff, 3 * CHUNK:4 * CHUNK]
        hi = slots[s, 1, 0:ff, 4 * CHUNK:5 * CHUNK]
        cols = pl.ds(pl.multiple_of(c * CHUNK, CHUNK), CHUNK)
        s_ref[:, cols] = (dot_f32(act_s[:, 0:ff], lo) + dot_f32(act_s[:, ff:2 * ff], hi)).astype(BF16)

        @pl.when(c + RING < chunks)
        def _():
            issue_down(c + RING, s)

    def combine_side(dst, slot, side):
        own = pl.ds(pl.multiple_of(side * (tokens // 2), tokens // 2), tokens // 2)
        for e in range(experts):
            part = tr_ref[own, experts + e:experts + e + 1] * dot_f32(q_all[e, own, :], e_ref[e])
            part = part.reshape(dst.shape[1:])
            if e == 0:
                dst[slot] = part
            else:
                dst[slot] = dst[slot] + part

    def combine(c):
        @pl.when(c >= 2)
        def _():
            send_d(c - 2).wait_send()

        combine_side(obuf, c % 2, 1 - core)
        send_d(c).start()
        combine_side(pbuf, c, core)

    def reduce_pair(c):
        send_d(c).wait_recv()
        pbuf[c] = pbuf[c] + dbuf[c % 2]
        for i in range(2):
            send_a(c, i).start()
        for i in range(2):
            send_b(c, i, i).start()

    def reduce_diag(c):
        for i in range(2):
            send_a(c, 1 - i).wait_recv()
            q = (xq, yq)[i]
            rest = slice((1 - i) * half, (2 - i) * half)
            pbuf[c, q, rest] = pbuf[c, q, rest] + abuf[c, 1 - i]
            send_b(c, i, 1 - i).start()

    def finish(c):
        cols = pl.ds(pl.multiple_of(c * CHUNK, CHUNK), CHUNK)
        local = y_ref[:, cols].astype(F32) + s_ref[:, cols].astype(F32)
        if not first:
            local = jnp.where(base == 0.0, local, 0.0)
        routed = pbuf[c, chip]
        for i in range(2):
            send_b(c, i).wait_recv()
            routed = routed + rbuf[c, i]

        @pl.when(c >= 2)
        def _():
            out_copy(c - 2).wait()

        out_ref[:, cols] = (local + routed).astype(out_ref.dtype)
        out_copy(c).start()

        @pl.when(c >= chunks - 2)
        def _():
            send_d(c).wait_send()

        for i in range(2):
            send_a(c, i).wait_send()
            send_b(c, i).wait_send()

    def stage_two(c, carry):
        pl.when(c < chunks)(lambda: down_project(c))
        pl.when(jnp.logical_and(c >= 1, c < chunks + 1))(lambda: reduce_pair(c - 1))
        pl.when(c < chunks)(lambda: combine(c))
        pl.when(jnp.logical_and(c >= 2, c < chunks + 2))(lambda: reduce_diag(c - 2))
        pl.when(c >= 4)(lambda: finish(c - 4))
        return carry

    lax.fori_loop(0, chunks + 4, stage_two, 0)

    def drain(c, carry):
        out_copy(c).wait()
        return carry

    lax.fori_loop(chunks - 2, chunks, drain, 0)


def moe_call(base, gain, wgt, idst, y, w1s, w3s, w2s, w1e, w3e, w2e):
    first = base is None
    rows, width = y.shape
    experts, _, ff = w1e.shape
    tokens = rows * 8
    chunks = width // CHUNK
    vmem = pl.BlockSpec(memory_space=pltpu.VMEM)
    hbm = pl.BlockSpec(memory_space=pl.ANY)
    dma = pltpu.SemaphoreType.DMA
    small = ([] if first else [base]) + [gain, wgt, idst]
    return pl.pallas_call(
        functools.partial(moe_kernel, first),
        out_shape=(jax.ShapeDtypeStruct((rows, width), BF16 if first else F32), jax.ShapeDtypeStruct((1, 1), F32)),
        in_specs=[vmem] * (len(small) + 1) + [hbm] * 6,
        out_specs=(hbm, hbm),
        scratch_shapes=[
            pltpu.VMEM((rows, width), BF16 if first else F32),
            pltpu.SMEM((1, 1), F32),
            pltpu.VMEM((RING, 2, width, ff), BF16),
            pltpu.VMEM((8, rows, width), BF16),
            pltpu.VMEM((8, 16, 128), F32),
            pltpu.VMEM((16, tokens), F32),
            pltpu.VMEM((2 * experts, tokens), F32),
            pltpu.VMEM((tokens, 128), F32),
            pltpu.VMEM((experts, tokens, CAP), BF16),
            pltpu.VMEM((2, CAP, width), BF16),
            pltpu.VMEM((experts, CAP, ff), BF16),
            pltpu.VMEM((rows, 2 * ff), BF16),
            pltpu.VMEM((chunks, 4, rows, CHUNK), F32),
            pltpu.VMEM((2, 4, rows, CHUNK), F32),
            pltpu.VMEM((2, 4, rows, CHUNK), F32),
            pltpu.VMEM((chunks, 2, rows // 2, CHUNK), F32),
            pltpu.VMEM((chunks, 2, rows, CHUNK), F32),
            pltpu.VMEM((rows, width), BF16),
            pltpu.VMEM((experts, CAP, CHUNK), BF16),
            dma((2,)),
            dma,
            dma((RING, 2)),
            dma((18,)),
            dma((18,)),
            dma((2,)),
            dma((2,)),
            dma((4, 2)),
            dma((4, 2)),
            dma((4, 2)),
            dma((chunks, 2)),
        ],
        compiler_params=pltpu.CompilerParams(
            collective_id=0 if first else 1, has_side_effects=True, vmem_limit_bytes=67_000_000),
    )(*small, y, w1s, w3s, w2s, w1e, w3e, w2e)


def solution(mesh):
    tok_spec = P(('dp', 'ep'), None)
    expert_spec = P('ep', None, None)

    def local_fn(hidden, norm_gain, w_gate, w1_shared, w3_shared, w2_shared, w1_experts, w3_experts, w2_experts, topk_ids):
        def routed_round(base):
            return moe_call(base, norm_gain, w_gate.T, topk_ids.T, hidden, w1_shared, w3_shared, w2_shared,
                            w1_experts, w3_experts, w2_experts)

        out, load = routed_round(None)

        def overflow(load, out):
            def add_round(i, acc):
                return acc + routed_round(jnp.full((8, 128), i * CAP, F32))[0]

            rounds = jnp.ceil(load / CAP).astype(jnp.int32)
            acc = lax.fori_loop(0, rounds, add_round, jnp.zeros(hidden.shape, F32))
            return acc.astype(BF16)

        return lax.cond(load[0, 0] > CAP, overflow, lambda load, out: out, load[0, 0], out)

    return jax.shard_map(local_fn, mesh=mesh, in_specs=(tok_spec, P(), P(), P(), P(), P(), expert_spec, expert_spec, expert_spec, tok_spec), out_specs=tok_spec, check_vma=False)
```

```python
import functools

import jax
import jax.numpy as jnp
from jax import lax
from jax.experimental import pallas as pl
from jax.experimental.pallas import tpu as pltpu
from jax.sharding import PartitionSpec as P

ROUTE_SCALE = 16
NORM_EPS = 1e-6
CAP = 128
CHUNK = 256
RING = 4
WIDE = 512
F32 = jnp.float32
BF16 = jnp.bfloat16


def dot_f32(lhs, rhs):
    return jnp.dot(lhs, rhs, preferred_element_type=F32)


def moe_kernel(first, *refs):
    if first:
        base = 0.0
    else:
        base, refs = refs[0][0:1, 0:1], refs[1:]
    (gain_ref, wgt_ref, idst_ref, y_ref, w1s, w3s, w2s, w1e, w3e, w2e,
     out_hbm, load_hbm,
     out_ref, load_ref, slots, ball, vall, vt_ref, rk_ref, tr_ref, q_all, xg_ref, act_ref, act_s,
     pbuf, obuf, dbuf, abuf, rbuf, s_ref, e_ref,
     out_sem, load_sem, wsem, ssem, rsem, ds_sem, dr_sem, as_sem, ar_sem, bs_sem, br_sem) = refs
    rows = y_ref.shape[0]
    half = rows // 2
    experts, _, ff = w1e.shape
    picks_per_row = idst_ref.shape[0]
    chunks = w2e.shape[2] // CHUNK
    tokens = rows * 8
    me = lax.axis_index("ep")
    core = me % 2
    chip = me // 2
    xpos = chip % 2
    ypos = chip // 2
    partner = me + 1 - 2 * core
    xdev = me + 2 - 4 * xpos
    ydev = me + 4 - 8 * ypos
    xq = chip + 1 - 2 * xpos
    yq = chip + 2 - 4 * ypos
    dq = 3 - chip
    diag = 2 * dq + core

    def issue_shared(part, s):
        cols = pl.ds(part * ff, ff)
        pltpu.make_async_copy(w1s.at[:, cols], slots.at[s, 0], wsem.at[s, 0]).start()
        pltpu.make_async_copy(w3s.at[:, cols], slots.at[s, 1], wsem.at[s, 1]).start()

    def issue_expert(e, s):
        pltpu.make_async_copy(w1e.at[e], slots.at[s, 0], wsem.at[s, 0]).start()
        pltpu.make_async_copy(w3e.at[e], slots.at[s, 1], wsem.at[s, 1]).start()

    def issue_down(c, s):
        cols = pl.ds(pl.multiple_of(c * CHUNK, CHUNK), CHUNK)
        for j in range(experts + 2):
            h, k = j // 5, j % 5
            src = w2e.at[j, :, cols] if j < experts else w2s.at[pl.ds((j - experts) * ff, ff), cols]
            dst = slots.at[s, h, pl.ds(0, ff), pl.ds(k * CHUNK, CHUNK)]
            pltpu.make_async_copy(src, dst, wsem.at[s, h]).start()

    def wait_full(s, h):
        pltpu.make_async_copy(w1e.at[0], slots.at[s, h], wsem.at[s, h]).wait()

    def wait_down(s, h):
        box = (pl.ds(0, ff), pl.ds(0, 5 * CHUNK))
        pltpu.make_async_copy(w1e.at[(0,) + box], slots.at[(s, h) + box], wsem.at[s, h]).wait()

    def up_project(lhs, s, dst, off):
        body = ff // CHUNK * CHUNK
        rest = ff - body
        for start in range(0, body, CHUNK):
            cols = slice(start, start + CHUNK)
            gate = dot_f32(lhs[...], slots[s, 0, :, cols])
            lin = dot_f32(lhs[...], slots[s, 1, :, cols])
            dst[:, off + start:off + start + CHUNK] = (jax.nn.silu(gate) * lin).astype(BF16)
        both = jnp.concatenate([slots[s, 0, :, body:ff], slots[s, 1, :, body:ff]], axis=1)
        both = dot_f32(lhs[...], both)
        dst[:, off + body:off + ff] = (jax.nn.silu(both[:, 0:rest]) * both[:, rest:]).astype(BF16)

    barrier = pltpu.get_barrier_semaphore()
    for dev in (partner, xdev, ydev, diag):
        pl.semaphore_signal(barrier, inc=1, device_id={"ep": dev}, device_id_type=pl.DeviceIdType.MESH)
    issue_shared(0, 0)
    issue_shared(1, 1)
    issue_expert(0, 2)
    issue_expert(1, 3)

    rows_f = y_ref[...].astype(F32)
    inv_rms = lax.rsqrt(jnp.mean(rows_f * rows_f, axis=-1, keepdims=True) + NORM_EPS)
    ball[me] = (rows_f * inv_rms * gain_ref[...].astype(F32).reshape(1, y_ref.shape[1])).astype(BF16)
    logits = lax.dot_general(wgt_ref[...], ball[me], (((1,), (1,)), ((), ())), preferred_element_type=F32)
    expv = jnp.exp(logits - jnp.max(logits, axis=0, keepdims=True))
    probs = expv / jnp.sum(expv, axis=0, keepdims=True)
    eid = lax.broadcasted_iota(jnp.int32, logits.shape, 0)
    vall[me] = jnp.full(vall.shape[1:], -1.0, F32)
    for j in range(picks_per_row):
        ids = idst_ref[j:j + 1, :]
        vall[me, j:j + 1, 0:rows] = ids.astype(F32)
        weight = jnp.sum(jnp.where(ids == eid, probs, 0.0), axis=0, keepdims=True)
        vall[me, 8 + j:9 + j, 0:rows] = ROUTE_SCALE * weight
    pl.semaphore_wait(barrier, 4)

    def same(t, ref, dev):
        return pltpu.make_async_remote_copy(
            src_ref=ref, dst_ref=ref, send_sem=ssem.at[t], recv_sem=rsem.at[t],
            device_id={"ep": dev}, device_id_type=pl.DeviceIdType.MESH)

    def block(dev, h=None):
        return ball.at[dev] if h is None else ball.at[dev, pl.ds(h * half, half)]

    x_v = same(0, vall.at[me], xdev)
    y_v = same(1, vall.at[me], ydev)
    p_v = same(2, vall.at[me], partner)
    d_v = same(8, vall.at[me], diag)
    x_h0 = same(3, block(me, 0), xdev)
    y_h1 = same(4, block(me, 1), ydev)
    x_h1 = same(5, block(me, 1), xdev)
    y_h0 = same(6, block(me, 0), ydev)
    p_own = same(7, block(me), partner)
    for cp in (x_v, y_v, d_v, p_v, x_h0, y_h1, x_h1, y_h0, p_own):
        cp.start()
    p_xv = same(9, vall.at[xdev], partner)
    p_yv = same(10, vall.at[ydev], partner)
    p_dv = same(11, vall.at[diag], partner)
    f_h0 = same(12, block(xdev, 0), ydev)
    f_h1 = same(13, block(ydev, 1), xdev)
    p_x = same(14, block(xdev), partner)
    p_y = same(15, block(ydev), partner)
    p_d0 = same(16, block(diag, 0), partner)
    p_d1 = same(17, block(diag, 1), partner)

    wait_full(0, 0)
    wait_full(0, 1)
    up_project(ball.at[me], 0, act_s, 0)
    issue_expert(2, 0)
    x_v.wait_recv()
    p_xv.start()
    y_v.wait_recv()
    p_yv.start()
    d_v.wait_recv()
    p_dv.start()
    x_h0.wait_recv()
    f_h0.start()
    y_h1.wait_recv()
    f_h1.start()

    wait_full(1, 0)
    wait_full(1, 1)
    up_project(ball.at[me], 1, act_s, ff)
    issue_expert(3, 1)
    for cp in (p_v, p_xv, p_yv, p_dv):
        cp.wait_recv()

    for k in range(8):
        vt_ref[:, k * rows:(k + 1) * rows] = vall[k, :, 0:rows]
    all_experts = wgt_ref.shape[0]
    every = lax.broadcasted_iota(jnp.int32, (all_experts, tokens), 0).astype(F32)
    hits = jnp.zeros((all_experts, tokens), F32)
    for j in range(picks_per_row):
        hits = hits + jnp.where(vt_ref[j:j + 1, :] == every, 1.0, 0.0)
    load_ref[0, 0] = jnp.max(jnp.sum(hits, axis=1, keepdims=True))
    load_copy = pltpu.make_async_copy(load_ref, load_hbm, load_sem)
    load_copy.start()
    local = (lax.broadcasted_iota(jnp.int32, (experts, tokens), 0) + me * experts).astype(F32)
    picks = jnp.zeros((experts, tokens), F32)
    weights = jnp.zeros((experts, tokens), F32)
    for j in range(picks_per_row):
        match = vt_ref[j:j + 1, :] == local
        picks = jnp.where(match, 1.0, picks)
        weights = jnp.where(match, vt_ref[8 + j:9 + j, :], weights)
    sel = picks > 0.5
    picks = jnp.concatenate([picks, picks], axis=0).astype(BF16)
    upper = lax.broadcasted_iota(jnp.int32, (tokens, tokens), 0) < lax.broadcasted_iota(jnp.int32, (tokens, tokens), 1)
    upper = jnp.where(upper, 1.0, 0.0).astype(BF16)
    rank = dot_f32(picks, upper)[0:experts] - base
    rank = jnp.where(sel, rank, -1.0)
    rk_ref[0:experts, :] = rank
    rk_ref[experts:2 * experts, :] = weights

    x_h1.wait_recv()
    p_x.start()
    y_h0.wait_recv()
    p_y.start()

    stacked = jnp.concatenate([rk_ref[...], jnp.zeros((128 - 2 * experts, tokens), F32)], axis=0).T
    for k in range(8):
        pos = (k % 2) * 4 + k // 2
        tr_ref[pos * rows:(pos + 1) * rows, :] = stacked[k * rows:(k + 1) * rows, :]
    lane = lax.broadcasted_iota(jnp.int32, (tokens, CAP), 1).astype(F32)
    for e in range(experts):
        q_all[e] = jnp.where(tr_ref[:, e:e + 1] == lane, 1.0, 0.0).astype(BF16)

    f_h0.wait_recv()
    p_d0.start()
    f_h1.wait_recv()
    p_d1.start()
    for cp in (p_own, p_x, p_y, p_d0, p_d1):
        cp.wait_recv()

    slot_row = lax.broadcasted_iota(jnp.int32, (CAP, tokens), 0).astype(F32)
    width = ball.shape[2]

    def gather(e):
        pick = jnp.where(rk_ref[pl.ds(e, 1), :] == slot_row, 1.0, 0.0).astype(BF16)
        for k in range(0, width, WIDE):
            xg_ref[e % 2, :, k:k + WIDE] = dot_f32(pick, ball[:, :, k:k + WIDE].reshape(tokens, WIDE)).astype(BF16)

    def stage_one(e, carry):
        s = (e + 2) % RING
        wait_full(s, 0)
        wait_full(s, 1)
        up_project(xg_ref.at[e % 2], s, act_ref.at[e], 0)
        gather(e + 1)

        @pl.when(e + RING < experts)
        def _():
            issue_expert(e + RING, s)

        @pl.when(e + RING >= experts)
        def _():
            issue_down(e + RING - experts, s)

        return carry

    gather(0)
    last = experts - 1
    lax.fori_loop(0, last, stage_one, 0)
    wait_full((last + 2) % RING, 0)
    wait_full((last + 2) % RING, 1)
    up_project(xg_ref.at[last % 2], (last + 2) % RING, act_ref.at[last], 0)
    issue_down(RING - 1, (last + 2) % RING)

    for cp in (x_v, y_v, d_v, p_v, x_h0, y_h1, x_h1, y_h0, p_own, p_xv, p_yv, p_dv, f_h0, f_h1, p_x, p_y, p_d0, p_d1):
        cp.wait_send()

    load_copy.wait()

    def send_d(c):
        return pltpu.make_async_remote_copy(
            src_ref=obuf.at[c % 2], dst_ref=dbuf.at[c % 2], send_sem=ds_sem.at[c % 2], recv_sem=dr_sem.at[c % 2],
            device_id={"ep": partner}, device_id_type=pl.DeviceIdType.MESH)

    def send_a(c, i):
        return pltpu.make_async_remote_copy(
            src_ref=pbuf.at[c, dq, pl.ds(i * half, half)], dst_ref=abuf.at[c, i],
            send_sem=as_sem.at[c % 4, i], recv_sem=ar_sem.at[c % 4, i],
            device_id={"ep": (xdev, ydev)[i]}, device_id_type=pl.DeviceIdType.MESH)

    def send_b(c, i, h=None):
        own = pl.ds(0, rows) if h is None else pl.ds(h * half, half)
        return pltpu.make_async_remote_copy(
            src_ref=pbuf.at[c, (xq, yq)[i], own], dst_ref=rbuf.at[c, i, own],
            send_sem=bs_sem.at[c % 4, i], recv_sem=br_sem.at[c, i],
            device_id={"ep": (xdev, ydev)[i]}, device_id_type=pl.DeviceIdType.MESH)

    def out_copy(c):
        cols = pl.ds(pl.multiple_of(c * CHUNK, CHUNK), CHUNK)
        return pltpu.make_async_copy(out_ref.at[:, cols], out_hbm.at[:, cols], out_sem.at[c % 2])

    def down_project(c):
        s = (c + experts + 2) % RING
        wait_down(s, 0)
        wait_down(s, 1)
        for e in range(experts):
            slab = slots[s, e // 5, 0:ff, (e % 5) * CHUNK:(e % 5 + 1) * CHUNK]
            e_ref[e] = dot_f32(act_ref[e], slab).astype(BF16)
        lo = slots[s, 1, 0:ff, 3 * CHUNK:4 * CHUNK]
        hi = slots[s, 1, 0:ff, 4 * CHUNK:5 * CHUNK]
        cols = pl.ds(pl.multiple_of(c * CHUNK, CHUNK), CHUNK)
        s_ref[:, cols] = (dot_f32(act_s[:, 0:ff], lo) + dot_f32(act_s[:, ff:2 * ff], hi)).astype(BF16)

        @pl.when(c + RING < chunks)
        def _():
            issue_down(c + RING, s)

    def combine_side(dst, slot, side):
        own = pl.ds(pl.multiple_of(side * (tokens // 2), tokens // 2), tokens // 2)
        for e in range(experts):
            part = tr_ref[own, experts + e:experts + e + 1] * dot_f32(q_all[e, own, :], e_ref[e])
            part = part.reshape(dst.shape[1:])
            if e == 0:
                dst[slot] = part
            else:
                dst[slot] = dst[slot] + part

    def combine(c):
        @pl.when(c >= 2)
        def _():
            send_d(c - 2).wait_send()

        combine_side(obuf, c % 2, 1 - core)
        send_d(c).start()
        combine_side(pbuf, c, core)

    def reduce_pair(c):
        send_d(c).wait_recv()
        pbuf[c] = pbuf[c] + dbuf[c % 2]
        for i in range(2):
            send_a(c, i).start()
        for i in range(2):
            send_b(c, i, i).start()

    def reduce_diag(c):
        for i in range(2):
            send_a(c, 1 - i).wait_recv()
            q = (xq, yq)[i]
            rest = slice((1 - i) * half, (2 - i) * half)
            pbuf[c, q, rest] = pbuf[c, q, rest] + abuf[c, 1 - i]
            send_b(c, i, 1 - i).start()

    def finish(c):
        cols = pl.ds(pl.multiple_of(c * CHUNK, CHUNK), CHUNK)
        local = y_ref[:, cols].astype(F32) + s_ref[:, cols].astype(F32)
        if not first:
            local = jnp.where(base == 0.0, local, 0.0)
        routed = pbuf[c, chip]
        for i in range(2):
            send_b(c, i).wait_recv()
            routed = routed + rbuf[c, i]

        @pl.when(c >= 2)
        def _():
            out_copy(c - 2).wait()

        out_ref[:, cols] = (local + routed).astype(out_ref.dtype)
        out_copy(c).start()

        @pl.when(c >= chunks - 2)
        def _():
            send_d(c).wait_send()

        for i in range(2):
            send_a(c, i).wait_send()
            send_b(c, i).wait_send()

    def stage_two(c, carry):
        pl.when(c < chunks)(lambda: down_project(c))
        pl.when(jnp.logical_and(c >= 1, c < chunks + 1))(lambda: reduce_pair(c - 1))
        pl.when(c < chunks)(lambda: combine(c))
        pl.when(jnp.logical_and(c >= 2, c < chunks + 2))(lambda: reduce_diag(c - 2))
        pl.when(c >= 4)(lambda: finish(c - 4))
        return carry

    lax.fori_loop(0, chunks + 4, stage_two, 0)

    def drain(c, carry):
        out_copy(c).wait()
        return carry

    lax.fori_loop(chunks - 2, chunks, drain, 0)


def moe_call(base, gain, wgt, idst, y, w1s, w3s, w2s, w1e, w3e, w2e):
    first = base is None
    rows, width = y.shape
    experts, _, ff = w1e.shape
    tokens = rows * 8
    chunks = width // CHUNK
    vmem = pl.BlockSpec(memory_space=pltpu.VMEM)
    hbm = pl.BlockSpec(memory_space=pl.ANY)
    dma = pltpu.SemaphoreType.DMA
    small = ([] if first else [base]) + [gain, wgt, idst]
    return pl.pallas_call(
        functools.partial(moe_kernel, first),
        out_shape=(jax.ShapeDtypeStruct((rows, width), BF16 if first else F32), jax.ShapeDtypeStruct((1, 1), F32)),
        in_specs=[vmem] * (len(small) + 1) + [hbm] * 6,
        out_specs=(hbm, hbm),
        scratch_shapes=[
            pltpu.VMEM((rows, width), BF16 if first else F32),
            pltpu.SMEM((1, 1), F32),
            pltpu.VMEM((RING, 2, width, ff), BF16),
            pltpu.VMEM((8, rows, width), BF16),
            pltpu.VMEM((8, 16, 128), F32),
            pltpu.VMEM((16, tokens), F32),
            pltpu.VMEM((2 * experts, tokens), F32),
            pltpu.VMEM((tokens, 128), F32),
            pltpu.VMEM((experts, tokens, CAP), BF16),
            pltpu.VMEM((2, CAP, width), BF16),
            pltpu.VMEM((experts, CAP, ff), BF16),
            pltpu.VMEM((rows, 2 * ff), BF16),
            pltpu.VMEM((chunks, 4, rows, CHUNK), F32),
            pltpu.VMEM((2, 4, rows, CHUNK), F32),
            pltpu.VMEM((2, 4, rows, CHUNK), F32),
            pltpu.VMEM((chunks, 2, rows // 2, CHUNK), F32),
            pltpu.VMEM((chunks, 2, rows, CHUNK), F32),
            pltpu.VMEM((rows, width), BF16),
            pltpu.VMEM((experts, CAP, CHUNK), BF16),
            dma((2,)),
            dma,
            dma((RING, 2)),
            dma((18,)),
            dma((18,)),
            dma((2,)),
            dma((2,)),
            dma((4, 2)),
            dma((4, 2)),
            dma((4, 2)),
            dma((chunks, 2)),
        ],
        compiler_params=pltpu.CompilerParams(
            collective_id=0 if first else 1, has_side_effects=True, vmem_limit_bytes=67_000_000),
    )(*small, y, w1s, w3s, w2s, w1e, w3e, w2e)


def solution(mesh):
    tok_spec = P(('dp', 'ep'), None)
    expert_spec = P('ep', None, None)

    def local_fn(hidden, norm_gain, w_gate, w1_shared, w3_shared, w2_shared, w1_experts, w3_experts, w2_experts, topk_ids):
        def routed_round(base):
            return moe_call(base, norm_gain, w_gate.T, topk_ids.T, hidden, w1_shared, w3_shared, w2_shared,
                            w1_experts, w3_experts, w2_experts)

        out, load = routed_round(None)

        def overflow(load, out):
            def add_round(i, acc):
                return acc + routed_round(jnp.full((8, 128), i * CAP, F32))[0]

            rounds = jnp.ceil(load / CAP).astype(jnp.int32)
            acc = lax.fori_loop(0, rounds, add_round, jnp.zeros(hidden.shape, F32))
            return acc.astype(BF16)

        return lax.cond(load[0, 0] > CAP, overflow, lambda load, out: out, load[0, 0], out)

    return jax.shard_map(local_fn, mesh=mesh, in_specs=(tok_spec, P(), P(), P(), P(), P(), expert_spec, expert_spec, expert_spec, tok_spec), out_specs=tok_spec, check_vma=False)
```

```python
import functools

import jax
import jax.numpy as jnp
from jax import lax
from jax.experimental import pallas as pl
from jax.experimental.pallas import tpu as pltpu
from jax.sharding import PartitionSpec as P

ROUTE_SCALE = 16
NORM_EPS = 1e-6
CAP = 128
CHUNK = 256
RING = 4
WIDE = 512
F32 = jnp.float32
BF16 = jnp.bfloat16


def dot_f32(lhs, rhs):
    return jnp.dot(lhs, rhs, preferred_element_type=F32)


def moe_kernel(first, *refs):
    if first:
        base = 0.0
    else:
        base, refs = refs[0][0:1, 0:1], refs[1:]
    (gain_ref, wgt_ref, idst_ref, y_ref, w1s, w3s, w2s, w1e, w3e, w2e,
     out_hbm, load_hbm,
     out_ref, load_ref, slots, ball, vall, vt_ref, rk_ref, tr_ref, q_all, xg_ref, act_ref, act_s,
     pbuf, obuf, dbuf, abuf, rbuf, s_ref, e_ref,
     out_sem, load_sem, wsem, ssem, rsem, ds_sem, dr_sem, as_sem, ar_sem, bs_sem, br_sem) = refs
    rows = y_ref.shape[0]
    half = rows // 2
    experts, _, ff = w1e.shape
    picks_per_row = idst_ref.shape[0]
    chunks = w2e.shape[2] // CHUNK
    tokens = rows * 8
    me = lax.axis_index("ep")
    core = me % 2
    chip = me // 2
    xpos = chip % 2
    ypos = chip // 2
    partner = me + 1 - 2 * core
    xdev = me + 2 - 4 * xpos
    ydev = me + 4 - 8 * ypos
    xq = chip + 1 - 2 * xpos
    yq = chip + 2 - 4 * ypos
    dq = 3 - chip
    diag = 2 * dq + core

    def issue_shared(part, s):
        cols = pl.ds(part * ff, ff)
        pltpu.make_async_copy(w1s.at[:, cols], slots.at[s, 0], wsem.at[s, 0]).start()
        pltpu.make_async_copy(w3s.at[:, cols], slots.at[s, 1], wsem.at[s, 1]).start()

    def issue_expert(e, s):
        pltpu.make_async_copy(w1e.at[e], slots.at[s, 0], wsem.at[s, 0]).start()
        pltpu.make_async_copy(w3e.at[e], slots.at[s, 1], wsem.at[s, 1]).start()

    def issue_down(c, s):
        cols = pl.ds(pl.multiple_of(c * CHUNK, CHUNK), CHUNK)
        for j in range(experts + 2):
            h, k = j // 5, j % 5
            src = w2e.at[j, :, cols] if j < experts else w2s.at[pl.ds((j - experts) * ff, ff), cols]
            dst = slots.at[s, h, pl.ds(0, ff), pl.ds(k * CHUNK, CHUNK)]
            pltpu.make_async_copy(src, dst, wsem.at[s, h]).start()

    def wait_full(s, h):
        pltpu.make_async_copy(w1e.at[0], slots.at[s, h], wsem.at[s, h]).wait()

    def wait_down(s, h):
        box = (pl.ds(0, ff), pl.ds(0, 5 * CHUNK))
        pltpu.make_async_copy(w1e.at[(0,) + box], slots.at[(s, h) + box], wsem.at[s, h]).wait()

    def up_project(lhs, s, dst, off):
        body = ff // CHUNK * CHUNK
        rest = ff - body
        for start in range(0, body, CHUNK):
            cols = slice(start, start + CHUNK)
            gate = dot_f32(lhs[...], slots[s, 0, :, cols])
            lin = dot_f32(lhs[...], slots[s, 1, :, cols])
            dst[:, off + start:off + start + CHUNK] = (jax.nn.silu(gate) * lin).astype(BF16)
        both = jnp.concatenate([slots[s, 0, :, body:ff], slots[s, 1, :, body:ff]], axis=1)
        both = dot_f32(lhs[...], both)
        dst[:, off + body:off + ff] = (jax.nn.silu(both[:, 0:rest]) * both[:, rest:]).astype(BF16)

    barrier = pltpu.get_barrier_semaphore()
    for dev in (partner, xdev, ydev, diag):
        pl.semaphore_signal(barrier, inc=1, device_id={"ep": dev}, device_id_type=pl.DeviceIdType.MESH)
    issue_shared(0, 0)
    issue_shared(1, 1)

    rows_f = y_ref[...].astype(F32)
    inv_rms = lax.rsqrt(jnp.mean(rows_f * rows_f, axis=-1, keepdims=True) + NORM_EPS)
    ball[me] = (rows_f * inv_rms * gain_ref[...].astype(F32).reshape(1, y_ref.shape[1])).astype(BF16)
    logits = lax.dot_general(wgt_ref[...], ball[me], (((1,), (1,)), ((), ())), preferred_element_type=F32)
    expv = jnp.exp(logits - jnp.max(logits, axis=0, keepdims=True))
    probs = expv / jnp.sum(expv, axis=0, keepdims=True)
    eid = lax.broadcasted_iota(jnp.int32, logits.shape, 0)
    vall[me] = jnp.full(vall.shape[1:], -1.0, F32)
    for j in range(picks_per_row):
        ids = idst_ref[j:j + 1, :]
        vall[me, j:j + 1, 0:rows] = ids.astype(F32)
        weight = jnp.sum(jnp.where(ids == eid, probs, 0.0), axis=0, keepdims=True)
        vall[me, 8 + j:9 + j, 0:rows] = ROUTE_SCALE * weight
    pl.semaphore_wait(barrier, 4)

    def same(t, ref, dev):
        return pltpu.make_async_remote_copy(
            src_ref=ref, dst_ref=ref, send_sem=ssem.at[t], recv_sem=rsem.at[t],
            device_id={"ep": dev}, device_id_type=pl.DeviceIdType.MESH)

    def block(dev, h=None):
        return ball.at[dev] if h is None else ball.at[dev, pl.ds(h * half, half)]

    x_v = same(0, vall.at[me], xdev)
    y_v = same(1, vall.at[me], ydev)
    p_v = same(2, vall.at[me], partner)
    d_v = same(8, vall.at[me], diag)
    x_h0 = same(3, block(me, 0), xdev)
    y_h1 = same(4, block(me, 1), ydev)
    x_h1 = same(5, block(me, 1), xdev)
    y_h0 = same(6, block(me, 0), ydev)
    p_own = same(7, block(me), partner)
    for cp in (x_v, y_v, d_v, p_v, x_h0, y_h1, x_h1, y_h0, p_own):
        cp.start()
    p_xv = same(9, vall.at[xdev], partner)
    p_yv = same(10, vall.at[ydev], partner)
    p_dv = same(11, vall.at[diag], partner)
    f_h0 = same(12, block(xdev, 0), ydev)
    f_h1 = same(13, block(ydev, 1), xdev)
    p_x = same(14, block(xdev), partner)
    p_y = same(15, block(ydev), partner)
    p_d0 = same(16, block(diag, 0), partner)
    p_d1 = same(17, block(diag, 1), partner)

    wait_full(0, 0)
    wait_full(0, 1)
    issue_expert(0, 2)
    issue_expert(1, 3)
    up_project(ball.at[me], 0, act_s, 0)
    issue_expert(2, 0)
    x_v.wait_recv()
    p_xv.start()
    y_v.wait_recv()
    p_yv.start()
    d_v.wait_recv()
    p_dv.start()
    x_h0.wait_recv()
    f_h0.start()
    y_h1.wait_recv()
    f_h1.start()

    wait_full(1, 0)
    wait_full(1, 1)
    up_project(ball.at[me], 1, act_s, ff)
    issue_expert(3, 1)
    for cp in (p_v, p_xv, p_yv, p_dv):
        cp.wait_recv()

    for k in range(8):
        vt_ref[:, k * rows:(k + 1) * rows] = vall[k, :, 0:rows]
    all_experts = wgt_ref.shape[0]
    every = lax.broadcasted_iota(jnp.int32, (all_experts, tokens), 0).astype(F32)
    hits = jnp.zeros((all_experts, tokens), F32)
    for j in range(picks_per_row):
        hits = hits + jnp.where(vt_ref[j:j + 1, :] == every, 1.0, 0.0)
    load_ref[0, 0] = jnp.max(jnp.sum(hits, axis=1, keepdims=True))
    load_copy = pltpu.make_async_copy(load_ref, load_hbm, load_sem)
    load_copy.start()
    local = (lax.broadcasted_iota(jnp.int32, (experts, tokens), 0) + me * experts).astype(F32)
    picks = jnp.zeros((experts, tokens), F32)
    weights = jnp.zeros((experts, tokens), F32)
    for j in range(picks_per_row):
        match = vt_ref[j:j + 1, :] == local
        picks = jnp.where(match, 1.0, picks)
        weights = jnp.where(match, vt_ref[8 + j:9 + j, :], weights)
    sel = picks > 0.5
    picks = jnp.concatenate([picks, picks], axis=0).astype(BF16)
    upper = lax.broadcasted_iota(jnp.int32, (tokens, tokens), 0) < lax.broadcasted_iota(jnp.int32, (tokens, tokens), 1)
    upper = jnp.where(upper, 1.0, 0.0).astype(BF16)
    rank = dot_f32(picks, upper)[0:experts] - base
    rank = jnp.where(sel, rank, -1.0)
    rk_ref[0:experts, :] = rank
    rk_ref[experts:2 * experts, :] = weights

    x_h1.wait_recv()
    p_x.start()
    y_h0.wait_recv()
    p_y.start()

    stacked = jnp.concatenate([rk_ref[...], jnp.zeros((128 - 2 * experts, tokens), F32)], axis=0).T
    for k in range(8):
        pos = (k % 2) * 4 + k // 2
        tr_ref[pos * rows:(pos + 1) * rows, :] = stacked[k * rows:(k + 1) * rows, :]
    lane = lax.broadcasted_iota(jnp.int32, (tokens, CAP), 1).astype(F32)
    for e in range(experts):
        q_all[e] = jnp.where(tr_ref[:, e:e + 1] == lane, 1.0, 0.0).astype(BF16)

    f_h0.wait_recv()
    p_d0.start()
    f_h1.wait_recv()
    p_d1.start()
    for cp in (p_own, p_x, p_y, p_d0, p_d1):
        cp.wait_recv()

    slot_row = lax.broadcasted_iota(jnp.int32, (CAP, tokens), 0).astype(F32)
    width = ball.shape[2]

    def gather(e):
        pick = jnp.where(rk_ref[pl.ds(e, 1), :] == slot_row, 1.0, 0.0).astype(BF16)
        for k in range(0, width, WIDE):
            xg_ref[e % 2, :, k:k + WIDE] = dot_f32(pick, ball[:, :, k:k + WIDE].reshape(tokens, WIDE)).astype(BF16)

    def stage_one(e, carry):
        s = (e + 2) % RING
        wait_full(s, 0)
        wait_full(s, 1)
        up_project(xg_ref.at[e % 2], s, act_ref.at[e], 0)
        gather(e + 1)

        @pl.when(e + RING < experts)
        def _():
            issue_expert(e + RING, s)

        @pl.when(e + RING >= experts)
        def _():
            issue_down(e + RING - experts, s)

        return carry

    gather(0)
    last = experts - 1
    lax.fori_loop(0, last, stage_one, 0)
    wait_full((last + 2) % RING, 0)
    wait_full((last + 2) % RING, 1)
    up_project(xg_ref.at[last % 2], (last + 2) % RING, act_ref.at[last], 0)
    issue_down(RING - 1, (last + 2) % RING)

    for cp in (x_v, y_v, d_v, p_v, x_h0, y_h1, x_h1, y_h0, p_own, p_xv, p_yv, p_dv, f_h0, f_h1, p_x, p_y, p_d0, p_d1):
        cp.wait_send()

    load_copy.wait()

    def send_d(c):
        return pltpu.make_async_remote_copy(
            src_ref=obuf.at[c % 2], dst_ref=dbuf.at[c % 2], send_sem=ds_sem.at[c % 2], recv_sem=dr_sem.at[c % 2],
            device_id={"ep": partner}, device_id_type=pl.DeviceIdType.MESH)

    def send_a(c, i):
        return pltpu.make_async_remote_copy(
            src_ref=pbuf.at[c, dq, pl.ds(i * half, half)], dst_ref=abuf.at[c, i],
            send_sem=as_sem.at[c % 4, i], recv_sem=ar_sem.at[c % 4, i],
            device_id={"ep": (xdev, ydev)[i]}, device_id_type=pl.DeviceIdType.MESH)

    def send_b(c, i, h=None):
        own = pl.ds(0, rows) if h is None else pl.ds(h * half, half)
        return pltpu.make_async_remote_copy(
            src_ref=pbuf.at[c, (xq, yq)[i], own], dst_ref=rbuf.at[c, i, own],
            send_sem=bs_sem.at[c % 4, i], recv_sem=br_sem.at[c, i],
            device_id={"ep": (xdev, ydev)[i]}, device_id_type=pl.DeviceIdType.MESH)

    def out_copy(c):
        cols = pl.ds(pl.multiple_of(c * CHUNK, CHUNK), CHUNK)
        return pltpu.make_async_copy(out_ref.at[:, cols], out_hbm.at[:, cols], out_sem.at[c % 2])

    def down_project(c):
        s = (c + experts + 2) % RING
        wait_down(s, 0)
        wait_down(s, 1)
        for e in range(experts):
            slab = slots[s, e // 5, 0:ff, (e % 5) * CHUNK:(e % 5 + 1) * CHUNK]
            e_ref[e] = dot_f32(act_ref[e], slab).astype(BF16)
        lo = slots[s, 1, 0:ff, 3 * CHUNK:4 * CHUNK]
        hi = slots[s, 1, 0:ff, 4 * CHUNK:5 * CHUNK]
        cols = pl.ds(pl.multiple_of(c * CHUNK, CHUNK), CHUNK)
        s_ref[:, cols] = (dot_f32(act_s[:, 0:ff], lo) + dot_f32(act_s[:, ff:2 * ff], hi)).astype(BF16)

        @pl.when(c + RING < chunks)
        def _():
            issue_down(c + RING, s)

    def combine_side(dst, slot, side):
        own = pl.ds(pl.multiple_of(side * (tokens // 2), tokens // 2), tokens // 2)
        for e in range(experts):
            part = tr_ref[own, experts + e:experts + e + 1] * dot_f32(q_all[e, own, :], e_ref[e])
            part = part.reshape(dst.shape[1:])
            if e == 0:
                dst[slot] = part
            else:
                dst[slot] = dst[slot] + part

    def combine(c):
        @pl.when(c >= 2)
        def _():
            send_d(c - 2).wait_send()

        combine_side(obuf, c % 2, 1 - core)
        send_d(c).start()
        combine_side(pbuf, c, core)

    def reduce_pair(c):
        send_d(c).wait_recv()
        pbuf[c] = pbuf[c] + dbuf[c % 2]
        for i in range(2):
            send_a(c, i).start()
        for i in range(2):
            send_b(c, i, i).start()

    def reduce_diag(c):
        for i in range(2):
            send_a(c, 1 - i).wait_recv()
            q = (xq, yq)[i]
            rest = slice((1 - i) * half, (2 - i) * half)
            pbuf[c, q, rest] = pbuf[c, q, rest] + abuf[c, 1 - i]
            send_b(c, i, 1 - i).start()

    def finish(c):
        cols = pl.ds(pl.multiple_of(c * CHUNK, CHUNK), CHUNK)
        local = y_ref[:, cols].astype(F32) + s_ref[:, cols].astype(F32)
        if not first:
            local = jnp.where(base == 0.0, local, 0.0)
        routed = pbuf[c, chip]
        for i in range(2):
            send_b(c, i).wait_recv()
            routed = routed + rbuf[c, i]

        @pl.when(c >= 2)
        def _():
            out_copy(c - 2).wait()

        out_ref[:, cols] = (local + routed).astype(out_ref.dtype)
        out_copy(c).start()

        @pl.when(c >= chunks - 2)
        def _():
            send_d(c).wait_send()

        for i in range(2):
            send_a(c, i).wait_send()
            send_b(c, i).wait_send()

    def stage_two(c, carry):
        pl.when(c < chunks)(lambda: down_project(c))
        pl.when(jnp.logical_and(c >= 1, c < chunks + 1))(lambda: reduce_pair(c - 1))
        pl.when(c < chunks)(lambda: combine(c))
        pl.when(jnp.logical_and(c >= 2, c < chunks + 2))(lambda: reduce_diag(c - 2))
        pl.when(c >= 4)(lambda: finish(c - 4))
        return carry

    lax.fori_loop(0, chunks + 4, stage_two, 0)

    def drain(c, carry):
        out_copy(c).wait()
        return carry

    lax.fori_loop(chunks - 2, chunks, drain, 0)


def moe_call(base, gain, wgt, idst, y, w1s, w3s, w2s, w1e, w3e, w2e):
    first = base is None
    rows, width = y.shape
    experts, _, ff = w1e.shape
    tokens = rows * 8
    chunks = width // CHUNK
    vmem = pl.BlockSpec(memory_space=pltpu.VMEM)
    hbm = pl.BlockSpec(memory_space=pl.ANY)
    dma = pltpu.SemaphoreType.DMA
    small = ([] if first else [base]) + [gain, wgt, idst]
    return pl.pallas_call(
        functools.partial(moe_kernel, first),
        out_shape=(jax.ShapeDtypeStruct((rows, width), BF16 if first else F32), jax.ShapeDtypeStruct((1, 1), F32)),
        in_specs=[vmem] * (len(small) + 1) + [hbm] * 6,
        out_specs=(hbm, hbm),
        scratch_shapes=[
            pltpu.VMEM((rows, width), BF16 if first else F32),
            pltpu.SMEM((1, 1), F32),
            pltpu.VMEM((RING, 2, width, ff), BF16),
            pltpu.VMEM((8, rows, width), BF16),
            pltpu.VMEM((8, 16, 128), F32),
            pltpu.VMEM((16, tokens), F32),
            pltpu.VMEM((2 * experts, tokens), F32),
            pltpu.VMEM((tokens, 128), F32),
            pltpu.VMEM((experts, tokens, CAP), BF16),
            pltpu.VMEM((2, CAP, width), BF16),
            pltpu.VMEM((experts, CAP, ff), BF16),
            pltpu.VMEM((rows, 2 * ff), BF16),
            pltpu.VMEM((chunks, 4, rows, CHUNK), F32),
            pltpu.VMEM((2, 4, rows, CHUNK), F32),
            pltpu.VMEM((2, 4, rows, CHUNK), F32),
            pltpu.VMEM((chunks, 2, rows // 2, CHUNK), F32),
            pltpu.VMEM((chunks, 2, rows, CHUNK), F32),
            pltpu.VMEM((rows, width), BF16),
            pltpu.VMEM((experts, CAP, CHUNK), BF16),
            dma((2,)),
            dma,
            dma((RING, 2)),
            dma((18,)),
            dma((18,)),
            dma((2,)),
            dma((2,)),
            dma((4, 2)),
            dma((4, 2)),
            dma((4, 2)),
            dma((chunks, 2)),
        ],
        compiler_params=pltpu.CompilerParams(
            collective_id=0 if first else 1, has_side_effects=True, vmem_limit_bytes=67_000_000),
    )(*small, y, w1s, w3s, w2s, w1e, w3e, w2e)


def solution(mesh):
    tok_spec = P(('dp', 'ep'), None)
    expert_spec = P('ep', None, None)

    def local_fn(hidden, norm_gain, w_gate, w1_shared, w3_shared, w2_shared, w1_experts, w3_experts, w2_experts, topk_ids):
        def routed_round(base):
            return moe_call(base, norm_gain, w_gate.T, topk_ids.T, hidden, w1_shared, w3_shared, w2_shared,
                            w1_experts, w3_experts, w2_experts)

        out, load = routed_round(None)

        def overflow(load, out):
            def add_round(i, acc):
                return acc + routed_round(jnp.full((8, 128), i * CAP, F32))[0]

            rounds = jnp.ceil(load / CAP).astype(jnp.int32)
            acc = lax.fori_loop(0, rounds, add_round, jnp.zeros(hidden.shape, F32))
            return acc.astype(BF16)

        return lax.cond(load[0, 0] > CAP, overflow, lambda load, out: out, load[0, 0], out)

    return jax.shard_map(local_fn, mesh=mesh, in_specs=(tok_spec, P(), P(), P(), P(), P(), expert_spec, expert_spec, expert_spec, tok_spec), out_specs=tok_spec, check_vma=False)
```
